256 devices in a mesh: rows: 64 (over y, z, core), grp: 4 (over x).
Axes of the slice: x: 4, y: 4, z: 8, core: 2. Of those that a mesh axis runs over, the one named last changes fastest.
Arguments:
- panel: float32 [65536, 256], P(('rows', 'grp')), may hold values from -6000 to 6000
- trailing: float32 [65536, 2048], P(('rows', 'grp')), may hold values from -6000 to 6000
Outputs:
- upper_panel: float32 [256, 256], replicated
- projection: float32 [256, 2048], replicated
- updated: float32 [65536, 2048], P(('rows', 'grp'))
- upper_next: float32 [256, 256], replicated
The draws below stay inside these ranges and needn't reach their ends.
All inputs are finite; a program needn't handle non-finite values.
Results may differ from the reference program's by a relative error of at most 0.00019.
Values sent between devices are 32-bit elements; how exact they have to be, the bound alone decides.
No kernel may reach another device: no remote copies, remote signals or barrier semaphores. Data moves between devices by JAX's collectives and lax.ppermute only.
A program may use at most 128 MiB of HBM per device.

```python
import math
import jax
import jax.numpy as jnp
from jax import lax

PB = 256
TC = 2048
NROWS = 65536


def row_scale(key):
    position = jnp.arange(NROWS, dtype=jnp.float32) / max(NROWS - 1, 1)
    jitter = jnp.exp(jax.random.uniform(jax.random.fold_in(key, 11), (NROWS, 1), jnp.float32, 0.0, math.log(10.0)))
    return (3.0 ** position)[:, None] * jitter


def mixed_block(key, salt):
    coupling = jax.random.normal(jax.random.fold_in(key, salt), (PB, PB), jnp.float32)
    return jnp.eye(PB, dtype=jnp.float32) + 0.25 * coupling / math.sqrt(PB)


def panel_values(key):
    normals = jax.random.normal(jax.random.fold_in(key, 1), (NROWS, PB), jnp.float32)
    values = jnp.dot(normals, mixed_block(key, 2), precision=lax.Precision.HIGHEST)
    spread = math.log(10.0)
    column_scale = jnp.exp(jax.random.uniform(jax.random.fold_in(key, 3), (PB,), jnp.float32, 0.0, spread))
    return values * column_scale * row_scale(key)


def draw_panel(key, part):
    return panel_values(key)


def draw_trailing(key, part):
    values = panel_values(key)
    loading = jax.random.normal(jax.random.fold_in(key, 5), (PB, TC), jnp.float32) / math.sqrt(PB)
    normals = jax.random.normal(jax.random.fold_in(key, 6), (NROWS, TC), jnp.float32)
    leading = jnp.dot(normals[:, :PB], mixed_block(key, 7), precision=lax.Precision.HIGHEST)
    noise_part = jnp.concatenate([leading, normals[:, PB:]], axis=1)
    spread = math.log(10.0)
    column_scale = jnp.exp(jax.random.uniform(jax.random.fold_in(key, 8), (TC,), jnp.float32, 0.0, spread))
    noise_part = noise_part * column_scale * row_scale(key)
    return jnp.dot(values, loading, precision=lax.Precision.HIGHEST) + noise_part


def setup_inputs(seed: int = 0) -> dict:
    splits = jax.random.split(jax.random.key(seed), 3)
    panel = draw_panel(jax.random.fold_in(splits[2], 71), 0)
    trailing = draw_trailing(jax.random.fold_in(splits[2], 71), 0)
    return {"panel": panel, "trailing": trailing}


def cross(left, right):
    return lax.dot_general(left.astype(jnp.float32), right.astype(jnp.float32), (((0,), (0,)), ((), ())), precision=lax.Precision.HIGHEST, preferred_element_type=jnp.float32)

def upper_of(matrix):
    return jnp.linalg.cholesky(matrix).T

def reference(panel, trailing):
    inv_rows = 1.0 / panel.shape[0]
    width = panel.shape[1]
    upper_panel = upper_of(cross(panel, panel) * inv_rows)
    inverse = lax.linalg.triangular_solve(upper_panel, jnp.eye(width, dtype=upper_panel.dtype), left_side=True, lower=False)
    ortho_basis = jnp.dot(panel.astype(jnp.float32), inverse.astype(jnp.float32), precision=lax.Precision.HIGHEST, preferred_element_type=jnp.float32)
    projection = cross(ortho_basis, trailing) * inv_rows
    updated = trailing - jnp.dot(ortho_basis.astype(jnp.float32), projection.astype(jnp.float32), precision=lax.Precision.HIGHEST, preferred_element_type=jnp.float32)
    leading = updated[:, :width]
    upper_next = upper_of(cross(leading, leading) * inv_rows)
    return (upper_panel, projection, updated, upper_next)
```

```python
import functools
import jax, jax.numpy as jnp
from jax import lax
from jax.experimental import pallas as pl
from jax.experimental.pallas import tpu as pltpu
from jax.sharding import Mesh, PartitionSpec as P

LANES = 128


def row_of(block, row):
    return jnp.broadcast_to(block[row:row + 1, :], block.shape)


def lane_of(block, lane):
    return jnp.broadcast_to(block[:, lane:lane + 1], block.shape)


def thirds(value):
    high = value.astype(jnp.bfloat16)
    rest = value - high.astype(jnp.float32)
    middle = rest.astype(jnp.bfloat16)
    low = (rest - middle.astype(jnp.float32)).astype(jnp.bfloat16)
    return high, middle, low


def outer(left, right):
    l1, l2, l3 = thirds(left)
    r1, r2, r3 = thirds(right)
    return lax.dot_general(
        jnp.concatenate([l1, l1, l2, l2, l1, l3], axis=0),
        jnp.concatenate([r1, r2, r1, r2, r3, r1], axis=0),
        (((0,), (0,)), ((), ())),
        preferred_element_type=jnp.float32,
    )


def factor(work, order, strip, extra, emit):
    groups = strip // 8
    sub_ids = lax.broadcasted_iota(jnp.int32, (8, LANES), 0)
    for start in range(0, order, strip):
        first = start // LANES
        stop = start + strip
        tiles = list(range(first, order // LANES))
        if extra:
            tiles += [order // LANES + t for t in range((stop + LANES - 1) // LANES)]
        rows = {
            (g, t): work[start + 8 * g:start + 8 * g + 8, LANES * t:LANES * t + LANES]
            for g in range(groups) for t in tiles
        }
        offset = start - LANES * first
        cols = {
            (m, g): lane_of(rows[g, first], offset + m)
            for m in range(strip) for g in range(m // 8, groups)
        }
        scale = [None] * groups
        for j in range(strip):
            g0, s0 = divmod(j, 8)
            inv_root = lax.rsqrt(row_of(cols[j, g0], s0))
            inv = inv_root * inv_root
            scale[g0] = inv_root if s0 == 0 else jnp.where(sub_ids == s0, inv_root, scale[g0])
            mult = {g: cols[j, g] * inv for g in range(g0, groups)}
            for m in range(j + 1, strip):
                entry = row_of(cols[j, m // 8], m % 8)
                for g in range(m // 8, groups):
                    cols[m, g] = cols[m, g] - mult[g] * entry
            if s0 == 7:
                del mult[g0]
            else:
                mult[g0] = jnp.where(sub_ids > s0, mult[g0], 0.0)
            for t in tiles:
                pivot_row = row_of(rows[g0, t], s0)
                for g in mult:
                    rows[g, t] = rows[g, t] - mult[g] * pivot_row
        for key in rows:
            rows[key] = rows[key] * scale[key[0]]
        block = {t: jnp.concatenate([rows[g, t] for g in range(groups)], axis=0) for t in tiles}
        emit(start, block)
        if stop == order:
            return
        base = stop // LANES
        left = jnp.concatenate([block[t] for t in range(base, order // LANES)], axis=1)
        keep = [t for t in tiles if t >= base]
        change = outer(left, jnp.concatenate([block[t] for t in keep], axis=1))
        for i, t in enumerate(keep):
            area = (slice(stop, order), slice(LANES * t, LANES * t + LANES))
            work[area] = work[area] - change[stop - LANES * base:, LANES * i:LANES * i + LANES]


def pair_kernel(strip, inv_rows, gram_ref, cross_ref, head_ref, upper_ref, inverse_ref, next_ref, work):
    order = gram_ref.shape[0]
    tiles = order // LANES
    row_ids = lax.broadcasted_iota(jnp.int32, (order, order), 0)
    col_ids = lax.broadcasted_iota(jnp.int32, (order, order), 1)
    work[:, :order] = gram_ref[...] * inv_rows
    work[:, order:] = jnp.where(row_ids == col_ids, 1.0, 0.0)
    upper_ref[...] = jnp.zeros_like(upper_ref)
    inverse_ref[...] = jnp.zeros_like(inverse_ref)
    next_ref[...] = jnp.zeros_like(next_ref)

    def emit_to(upper, inverse):
        def emit(start, block):
            ids = lax.broadcasted_iota(jnp.int32, (strip, LANES), 0) + start
            lanes = lax.broadcasted_iota(jnp.int32, (strip, LANES), 1)
            for t, value in block.items():
                if t < tiles:
                    value = jnp.where(lanes + LANES * t >= ids, value, 0.0)
                    upper[start:start + strip, LANES * t:LANES * t + LANES] = value
                else:
                    inverse[start:start + strip, LANES * (t - tiles):LANES * (t - tiles) + LANES] = value
        return emit

    factor(work, order, strip, True, emit_to(upper_ref, inverse_ref))
    dot = functools.partial(lax.dot_general, precision=lax.Precision.HIGHEST, preferred_element_type=jnp.float32)
    proj = dot(inverse_ref[...], cross_ref[...] * inv_rows, (((1,), (0,)), ((), ())))
    work[:, :order] = head_ref[...] * inv_rows - dot(proj, proj, (((0,), (0,)), ((), ())))
    factor(work, order, strip, False, emit_to(next_ref, None))


def factor_two(gram, cross, head, inv_rows, strip=16):
    order = gram.shape[0]
    shape = jax.ShapeDtypeStruct((order, order), jnp.float32)
    vmem = pl.BlockSpec(memory_space=pltpu.VMEM)
    return pl.pallas_call(
        functools.partial(pair_kernel, strip, inv_rows),
        out_shape=(shape, shape, shape),
        in_specs=[vmem] * 3,
        out_specs=(vmem,) * 3,
        scratch_shapes=[pltpu.VMEM((order, 2 * order), jnp.float32)],
        cost_estimate=pl.CostEstimate(flops=18 * 10**9, bytes_accessed=6 * 4 * order**2, transcendentals=0),
    )(gram, cross, head)


def cross(left, right):
    return lax.dot_general(
        left,
        right,
        (((0,), (0,)), ((), ())),
        precision=lax.Precision.HIGHEST,
        preferred_element_type=jnp.float32,
    )


def product(left, right):
    return jnp.dot(left, right, precision=lax.Precision.HIGHEST, preferred_element_type=jnp.float32)


def spread(block, axes):
    copies = jnp.broadcast_to(block[None], (lax.axis_size(axes),) + block.shape)
    return lax.all_to_all(copies, axes, 0, 0, tiled=True)


def swap_cores(value):
    return lax.ppermute(value, "core", ((0, 1), (1, 0)))


def gather_pieces(value):
    rows, width = value.shape
    core = lax.axis_index("core")
    halves = value.reshape(2, rows // 2, width)
    mine = lax.dynamic_index_in_dim(halves, core, 0, keepdims=False)
    other = lax.dynamic_index_in_dim(halves, 1 - core, 0, keepdims=False)
    mine = mine + swap_cores(other)
    plane = ("y", "x")
    pieces = mine.reshape(lax.axis_size(plane), -1, width)
    piece = jnp.sum(lax.all_to_all(pieces, plane, 0, 0, tiled=True), axis=0)
    piece = jnp.sum(spread(piece, ("z",)), axis=0)
    return spread(piece, plane).reshape(rows // 2, width)


def join_halves(mine):
    other = swap_cores(mine)
    first = lax.axis_index("core") == 0
    return jnp.concatenate([jnp.where(first, mine, other), jnp.where(first, other, mine)], axis=0)


def per_device(panel, trailing):
    inv_rows = 1.0 / (panel.shape[0] * lax.axis_size(("y", "z", "core", "x")))
    width = panel.shape[1]
    head = trailing[:, :width]
    grams = join_halves(gather_pieces(
        jnp.concatenate([cross(panel, panel), cross(panel, head), cross(head, head)], axis=1)
    ))
    rest_half = gather_pieces(cross(panel, trailing[:, width:]))
    cross_head = grams[:, width:2 * width]
    upper_panel, lower_inv, upper_next = factor_two(
        grams[:, :width], cross_head, grams[:, 2 * width:], inv_rows
    )
    rest_half, lower_inv = lax.optimization_barrier((rest_half, lower_inv))
    cross_terms = jnp.concatenate([cross_head, join_halves(rest_half)], axis=1)
    projection = product(lower_inv, cross_terms) * inv_rows
    ortho_basis = product(panel, lower_inv.T)
    updated = trailing - product(ortho_basis, projection)
    return (upper_panel, projection, updated, upper_next)


def solution(mesh):
    chips = Mesh(mesh.devices.reshape(4, 8, 2, 4), ("y", "z", "core", "x"))
    rows = ("y", "z", "core", "x")
    return jax.shard_map(
        per_device,
        mesh=chips,
        in_specs=(P(rows, None), P(rows, None)),
        out_specs=(P(), P(), P(rows, None), P()),
        check_vma=False,
    )
```

```python
import functools
import jax, jax.numpy as jnp
from jax import lax
from jax.experimental import pallas as pl
from jax.experimental.pallas import tpu as pltpu
from jax.sharding import Mesh, PartitionSpec as P

LANES = 128
VMEM_BYTES = 16 * 2**20
VMEM = pl.BlockSpec(memory_space=pltpu.VMEM)


def row_of(block, row):
    return jnp.broadcast_to(block[row:row + 1, :], block.shape)


def lane_of(block, lane):
    return jnp.broadcast_to(block[:, lane:lane + 1], block.shape)


def thirds(value):
    high = value.astype(jnp.bfloat16)
    rest = value - high.astype(jnp.float32)
    middle = rest.astype(jnp.bfloat16)
    low = (rest - middle.astype(jnp.float32)).astype(jnp.bfloat16)
    return high, middle, low


def matmul(left, right):
    l1, l2, l3 = left
    r1, r2, r3 = right
    pairs = ((l1, r3), (l3, r1), (l2, r2), (l1, r2), (l2, r1), (l1, r1))
    return sum(jnp.dot(a, b, preferred_element_type=jnp.float32) for a, b in pairs)


def outer(left, right):
    l1, l2, l3 = thirds(left)
    r1, r2, r3 = thirds(right)
    return lax.dot_general(
        jnp.concatenate([l1, l1, l2, l2, l1, l3], axis=0),
        jnp.concatenate([r1, r2, r1, r2, r3, r1], axis=0),
        (((0,), (0,)), ((), ())),
        preferred_element_type=jnp.float32,
    )


def factor(work, order, strip, extra, emit):
    groups = strip // 8
    sub_ids = lax.broadcasted_iota(jnp.int32, (8, LANES), 0)
    for start in range(0, order, strip):
        first = start // LANES
        stop = start + strip
        tiles = list(range(first, order // LANES))
        if extra:
            tiles += [order // LANES + t for t in range((stop + LANES - 1) // LANES)]
        rows = {
            (g, t): work[start + 8 * g:start + 8 * g + 8, LANES * t:LANES * t + LANES]
            for g in range(groups) for t in tiles
        }
        offset = start - LANES * first
        cols = {
            (m, g): lane_of(rows[g, first], offset + m)
            for m in range(strip) for g in range(m // 8, groups)
        }
        scale = [None] * groups
        for j in range(strip):
            g0, s0 = divmod(j, 8)
            inv_root = lax.rsqrt(row_of(cols[j, g0], s0))
            inv = inv_root * inv_root
            scale[g0] = inv_root if s0 == 0 else jnp.where(sub_ids == s0, inv_root, scale[g0])
            mult = {g: cols[j, g] * inv for g in range(g0, groups)}
            for m in range(j + 1, strip):
                entry = row_of(cols[j, m // 8], m % 8)
                for g in range(m // 8, groups):
                    cols[m, g] = cols[m, g] - mult[g] * entry
            if s0 == 7:
                del mult[g0]
            else:
                mult[g0] = jnp.where(sub_ids > s0, mult[g0], 0.0)
            for t in tiles:
                pivot_row = row_of(rows[g0, t], s0)
                for g in mult:
                    rows[g, t] = rows[g, t] - mult[g] * pivot_row
        for key in rows:
            rows[key] = rows[key] * scale[key[0]]
        block = {t: jnp.concatenate([rows[g, t] for g in range(groups)], axis=0) for t in tiles}
        emit(start, block)
        if stop == order:
            return
        base = stop // LANES
        left = jnp.concatenate([block[t] for t in range(base, order // LANES)], axis=1)
        keep = [t for t in tiles if t >= base]
        change = outer(left, jnp.concatenate([block[t] for t in keep], axis=1))
        for i, t in enumerate(keep):
            area = (slice(stop, order), slice(LANES * t, LANES * t + LANES))
            work[area] = work[area] - change[stop - LANES * base:, LANES * i:LANES * i + LANES]


def ordered(first, mine, other):
    return jnp.where(first, mine, other), jnp.where(first, other, mine)


def products_kernel(panel_ref, trailing_ref, mine_ref, other_ref):
    first = lax.axis_index("core") == 0
    width = panel_ref.shape[1]
    half = width // 2
    count = trailing_ref.shape[1] // width
    panel = panel_ref[...]
    head = trailing_ref[:, :width]
    left_panel = thirds(panel.T)
    left_head = thirds(head.T)
    for tile in range(count + 2):
        source = panel if tile == 0 else head if tile > count else trailing_ref[:, width * (tile - 1):width * tile]
        result = matmul(left_head if tile > count else left_panel, thirds(source))
        area = slice(width * tile, width * tile + width)
        mine_ref[:, area], other_ref[:, area] = ordered(first, result[:half], result[half:])


def products(panel, trailing):
    rows, width = panel.shape
    total = trailing.shape[1] + 2 * width
    shape = jax.ShapeDtypeStruct((width // 2, total), jnp.float32)
    return pl.pallas_call(
        products_kernel,
        out_shape=(shape, shape),
        in_specs=[VMEM] * 2,
        out_specs=(VMEM,) * 2,
        compiler_params=pltpu.CompilerParams(vmem_limit_bytes=VMEM_BYTES),
        cost_estimate=pl.CostEstimate(flops=12 * rows * width * total, bytes_accessed=8 * rows * total, transcendentals=0),
    )(panel, trailing)


def pair_kernel(strip, inv_rows, mine_ref, other_ref, upper_ref, inverse_ref, next_ref, work):
    order = upper_ref.shape[0]
    half = order // 2
    tiles = order // LANES
    first = lax.axis_index("core") == 0
    row_ids = lax.broadcasted_iota(jnp.int32, (order, order), 0)
    col_ids = lax.broadcasted_iota(jnp.int32, (order, order), 1)

    def block(index):
        area = slice(order * index, order * index + order)
        return jnp.concatenate(ordered(first, mine_ref[:, area], other_ref[:, area]), axis=0) * inv_rows

    work[:, :order] = block(0)
    work[:, order:] = jnp.where(row_ids == col_ids, 1.0, 0.0)
    upper_ref[...] = jnp.zeros_like(upper_ref)
    inverse_ref[...] = jnp.zeros_like(inverse_ref)
    next_ref[...] = jnp.zeros_like(next_ref)

    def emit_to(upper, inverse):
        def emit(start, block):
            ids = lax.broadcasted_iota(jnp.int32, (strip, LANES), 0) + start
            lanes = lax.broadcasted_iota(jnp.int32, (strip, LANES), 1)
            for t, value in block.items():
                if t < tiles:
                    value = jnp.where(lanes + LANES * t >= ids, value, 0.0)
                    upper[start:start + strip, LANES * t:LANES * t + LANES] = value
                else:
                    inverse[start:start + strip, LANES * (t - tiles):LANES * (t - tiles) + LANES] = value
        return emit

    factor(work, order, strip, True, emit_to(upper_ref, inverse_ref))
    proj = matmul(thirds(inverse_ref[...]), thirds(block(1)))
    work[:, :order] = block(2) - matmul(thirds(proj.T), thirds(proj))
    factor(work, order, strip, False, emit_to(next_ref, None))


def factor_two(mine, other, inv_rows, strip=16):
    order = mine.shape[1] // 3
    shape = jax.ShapeDtypeStruct((order, order), jnp.float32)
    return pl.pallas_call(
        functools.partial(pair_kernel, strip, inv_rows),
        out_shape=(shape, shape, shape),
        in_specs=[VMEM] * 2,
        out_specs=(VMEM,) * 3,
        scratch_shapes=[pltpu.VMEM((order, 2 * order), jnp.float32)],
        compiler_params=pltpu.CompilerParams(vmem_limit_bytes=VMEM_BYTES),
        cost_estimate=pl.CostEstimate(flops=18 * 10**9, bytes_accessed=6 * 4 * order**2, transcendentals=0),
    )(mine, other)


def update_kernel(
    inv_rows, panel_ref, inverse_ref, head_mine, head_other, rest_mine, rest_other, trailing_ref,
    proj_ref, updated_ref, inv_parts, basis_parts,
):
    step = pl.program_id(0)
    first = lax.axis_index("core") == 0

    @pl.when(step == 0)
    def _():
        inverse = inverse_ref[...]
        for index, part in enumerate(thirds(inverse)):
            inv_parts[index] = part
        basis = matmul(thirds(panel_ref[...]), thirds(inverse.T))
        for index, part in enumerate(thirds(basis)):
            basis_parts[index] = part

    mine = jnp.where(step == 0, head_mine[...], rest_mine[...])
    other = jnp.where(step == 0, head_other[...], rest_other[...])
    terms = jnp.concatenate(ordered(first, mine, other), axis=0) * inv_rows
    proj = matmul([inv_parts[i] for i in range(3)], thirds(terms))
    proj_ref[...] = proj
    updated_ref[...] = trailing_ref[...] - matmul([basis_parts[i] for i in range(3)], thirds(proj))


def update(panel, inverse, grams, rest, trailing, inv_rows):
    rows, width = panel.shape
    half = width // 2
    columns = trailing.shape[1]
    whole = pl.BlockSpec((width, width), lambda j: (0, 0))
    head = pl.BlockSpec((half, width), lambda j: (0, 1))
    tail = pl.BlockSpec((half, width), lambda j: (0, jnp.maximum(j - 1, 0)))
    column = pl.BlockSpec((rows, width), lambda j: (0, j))
    return pl.pallas_call(
        functools.partial(update_kernel, inv_rows),
        grid=(columns // width,),
        out_shape=(
            jax.ShapeDtypeStruct((width, columns), jnp.float32),
            jax.ShapeDtypeStruct((rows, columns), jnp.float32),
        ),
        in_specs=[whole, whole, head, head, tail, tail, column],
        out_specs=(column, column),
        scratch_shapes=[
            pltpu.VMEM((3, width, width), jnp.bfloat16),
            pltpu.VMEM((3, rows, width), jnp.bfloat16),
        ],
        compiler_params=pltpu.CompilerParams(vmem_limit_bytes=VMEM_BYTES),
        cost_estimate=pl.CostEstimate(flops=24 * rows * width * columns, bytes_accessed=16 * rows * columns, transcendentals=0),
    )(panel, inverse, *grams, *rest, trailing)


def spread(block, axes):
    copies = jnp.broadcast_to(block[None], (lax.axis_size(axes),) + block.shape)
    return lax.all_to_all(copies, axes, 0, 0, tiled=True)


def swap_cores(value):
    return lax.ppermute(value, "core", ((0, 1), (1, 0)))


def per_device(panel, trailing):
    inv_rows = 1.0 / (panel.shape[0] * lax.axis_size(("y", "z", "core", "x")))
    width = panel.shape[1]
    half = width // 2
    columns = trailing.shape[1]
    plane = ("y", "x")
    mine, other = products(panel, trailing)
    mine = mine + swap_cores(other)
    pieces = mine.reshape(lax.axis_size(plane), -1, mine.shape[1])
    piece = jnp.sum(lax.all_to_all(pieces, plane, 0, 0, tiled=True), axis=0)
    piece = jnp.sum(spread(piece, ("z",)), axis=0)
    first_part = jnp.concatenate([piece[:, :2 * width], piece[:, columns + width:]], axis=1)
    grams = spread(first_part, plane).reshape(half, -1)
    grams_other = swap_cores(grams)
    rest = spread(piece[:, 2 * width:columns + width], plane).reshape(half, -1)
    upper_panel, lower_inv, upper_next = factor_two(grams, grams_other, inv_rows)
    rest, lower_inv = lax.optimization_barrier((rest, lower_inv))
    projection, updated = update(
        panel, lower_inv, (grams, grams_other), (rest, swap_cores(rest)), trailing, inv_rows
    )
    return (upper_panel, projection, updated, upper_next)


def solution(mesh):
    chips = Mesh(mesh.devices.reshape(4, 8, 2, 4), ("y", "z", "core", "x"))
    rows = ("y", "z", "core", "x")
    return jax.shard_map(
        per_device,
        mesh=chips,
        in_specs=(P(rows, None), P(rows, None)),
        out_specs=(P(), P(), P(rows, None), P()),
        check_vma=False,
    )
```

```python
import functools
import jax, jax.numpy as jnp
from jax import lax
from jax.experimental import pallas as pl
from jax.experimental.pallas import tpu as pltpu
from jax.sharding import Mesh, PartitionSpec as P

LANES = 128
VMEM_BYTES = 16 * 2**20
VMEM = pl.BlockSpec(memory_space=pltpu.VMEM)
HBM = pl.BlockSpec(memory_space=pltpu.HBM)


in_hbm = functools.partial(pltpu.with_memory_space_constraint, memory_space=pltpu.HBM)


def row_of(block, row):
    return jnp.broadcast_to(block[row:row + 1, :], block.shape)


def lane_of(block, lane):
    return jnp.broadcast_to(block[:, lane:lane + 1], block.shape)


def thirds(value):
    high = value.astype(jnp.bfloat16)
    rest = value - high.astype(jnp.float32)
    middle = rest.astype(jnp.bfloat16)
    low = (rest - middle.astype(jnp.float32)).astype(jnp.bfloat16)
    return high, middle, low


def matmul(left, right):
    l1, l2, l3 = left
    r1, r2, r3 = right
    pairs = ((l1, r3), (l3, r1), (l2, r2), (l1, r2), (l2, r1), (l1, r1))
    return sum(jnp.dot(a, b, preferred_element_type=jnp.float32) for a, b in pairs)


def outer(left, right):
    l1, l2, l3 = thirds(left)
    r1, r2, r3 = thirds(right)
    return lax.dot_general(
        jnp.concatenate([l1, l1, l2, l2, l1, l3], axis=0),
        jnp.concatenate([r1, r2, r1, r2, r3, r1], axis=0),
        (((0,), (0,)), ((), ())),
        preferred_element_type=jnp.float32,
    )


def factor(work, order, strip, extra, emit):
    groups = strip // 8
    sub_ids = lax.broadcasted_iota(jnp.int32, (8, LANES), 0)
    for start in range(0, order, strip):
        first = start // LANES
        stop = start + strip
        tiles = list(range(first, order // LANES))
        if extra:
            tiles += [order // LANES + t for t in range((stop + LANES - 1) // LANES)]
        rows = {
            (g, t): work[start + 8 * g:start + 8 * g + 8, LANES * t:LANES * t + LANES]
            for g in range(groups) for t in tiles
        }
        offset = start - LANES * first
        cols = {
            (m, g): lane_of(rows[g, first], offset + m)
            for m in range(strip) for g in range(m // 8, groups)
        }
        scale = [None] * groups
        for j in range(strip):
            g0, s0 = divmod(j, 8)
            inv_root = lax.rsqrt(row_of(cols[j, g0], s0))
            inv = inv_root * inv_root
            scale[g0] = inv_root if s0 == 0 else jnp.where(sub_ids == s0, inv_root, scale[g0])
            mult = {g: cols[j, g] * inv for g in range(g0, groups)}
            for m in range(j + 1, strip):
                entry = row_of(cols[j, m // 8], m % 8)
                for g in range(m // 8, groups):
                    cols[m, g] = cols[m, g] - mult[g] * entry
            if s0 == 7:
                del mult[g0]
            else:
                mult[g0] = jnp.where(sub_ids > s0, mult[g0], 0.0)
            for t in tiles:
                pivot_row = row_of(rows[g0, t], s0)
                for g in mult:
                    rows[g, t] = rows[g, t] - mult[g] * pivot_row
        for key in rows:
            rows[key] = rows[key] * scale[key[0]]
        block = {t: jnp.concatenate([rows[g, t] for g in range(groups)], axis=0) for t in tiles}
        emit(start, block)
        if stop == order:
            return
        base = stop // LANES
        left = jnp.concatenate([block[t] for t in range(base, order // LANES)], axis=1)
        keep = [t for t in tiles if t >= base]
        change = outer(left, jnp.concatenate([block[t] for t in keep], axis=1))
        for i, t in enumerate(keep):
            area = (slice(stop, order), slice(LANES * t, LANES * t + LANES))
            work[area] = work[area] - change[stop - LANES * base:, LANES * i:LANES * i + LANES]


def ordered(first, mine, other):
    return jnp.where(first, mine, other), jnp.where(first, other, mine)


def products_kernel(panel_hbm, trailing_hbm, mine_ref, other_ref, panel_ref, trailing_ref, arrived):
    first = lax.axis_index("core") == 0
    width = panel_ref.shape[1]
    half = width // 2
    count = trailing_ref.shape[1] // width
    areas = [slice(width * t, width * t + width) for t in range(count + 2)]
    loads = [pltpu.make_async_copy(panel_hbm, panel_ref, arrived.at[0])]
    for t in range(count):
        loads.append(pltpu.make_async_copy(
            trailing_hbm.at[:, areas[t]], trailing_ref.at[:, areas[t]], arrived.at[t + 1]
        ))
    for load in loads:
        load.start()
    loads[0].wait()
    panel = panel_ref[...]
    left_panel = thirds(panel.T)
    for tile in range(count + 2):
        left = left_panel
        if tile == 0:
            source = panel
        elif tile <= count:
            loads[tile].wait()
            source = trailing_ref[:, areas[tile - 1]]
        else:
            source = trailing_ref[:, areas[0]]
            left = thirds(source.T)
        result = matmul(left, thirds(source))
        mine_ref[:, areas[tile]], other_ref[:, areas[tile]] = ordered(first, result[:half], result[half:])


def products(panel, trailing):
    rows, width = panel.shape
    total = trailing.shape[1] + 2 * width
    shape = jax.ShapeDtypeStruct((width // 2, total), jnp.float32)
    return pl.pallas_call(
        products_kernel,
        out_shape=(shape, shape),
        in_specs=[HBM] * 2,
        out_specs=(VMEM,) * 2,
        scratch_shapes=[
            pltpu.VMEM(panel.shape, jnp.float32),
            pltpu.VMEM(trailing.shape, jnp.float32),
            pltpu.SemaphoreType.DMA((trailing.shape[1] // width + 1,)),
        ],
        compiler_params=pltpu.CompilerParams(vmem_limit_bytes=VMEM_BYTES),
        cost_estimate=pl.CostEstimate(flops=12 * rows * width * total, bytes_accessed=8 * rows * total, transcendentals=0),
    )(in_hbm(panel), in_hbm(trailing))


def pair_kernel(
    strip, inv_rows, mine_ref, other_ref, panel_hbm, upper_ref, next_ref, parts_hbm,
    panel_ref, parts_ref, inverse_ref, work, moved,
):
    load = pltpu.make_async_copy(panel_hbm, panel_ref, moved.at[0])
    load.start()
    store = pltpu.make_async_copy(parts_ref, parts_hbm, moved.at[1])
    order = upper_ref.shape[0]
    half = order // 2
    tiles = order // LANES
    first = lax.axis_index("core") == 0
    row_ids = lax.broadcasted_iota(jnp.int32, (order, order), 0)
    col_ids = lax.broadcasted_iota(jnp.int32, (order, order), 1)

    def block(index):
        area = slice(order * index, order * index + order)
        return jnp.concatenate(ordered(first, mine_ref[:, area], other_ref[:, area]), axis=0) * inv_rows

    work[:, :order] = block(0)
    work[:, order:] = jnp.where(row_ids == col_ids, 1.0, 0.0)
    upper_ref[...] = jnp.zeros_like(upper_ref)
    inverse_ref[...] = jnp.zeros_like(inverse_ref)
    next_ref[...] = jnp.zeros_like(next_ref)

    def emit_to(upper, inverse):
        def emit(start, block):
            ids = lax.broadcasted_iota(jnp.int32, (strip, LANES), 0) + start
            lanes = lax.broadcasted_iota(jnp.int32, (strip, LANES), 1)
            for t, value in block.items():
                if t < tiles:
                    value = jnp.where(lanes + LANES * t >= ids, value, 0.0)
                    upper[start:start + strip, LANES * t:LANES * t + LANES] = value
                else:
                    inverse[start:start + strip, LANES * (t - tiles):LANES * (t - tiles) + LANES] = value
        return emit

    factor(work, order, strip, True, emit_to(upper_ref, inverse_ref))
    inverse = thirds(inverse_ref[...])
    for index, part in enumerate(inverse):
        parts_ref[index] = part
    load.wait()
    basis = matmul(thirds(panel_ref[...]), thirds(inverse_ref[...].T))
    for index, part in enumerate(thirds(basis)):
        parts_ref[3 + index] = part
    store.start()
    proj = matmul(inverse, thirds(block(1)))
    work[:, :order] = block(2) - matmul(thirds(proj.T), thirds(proj))
    factor(work, order, strip, False, emit_to(next_ref, None))
    store.wait()


def factor_two(mine, other, panel, inv_rows, strip=16):
    rows, order = panel.shape
    shape = jax.ShapeDtypeStruct((order, order), jnp.float32)
    return pl.pallas_call(
        functools.partial(pair_kernel, strip, inv_rows),
        out_shape=(
            shape,
            shape,
            pltpu.HBM((6, order, order), jnp.bfloat16),
        ),
        in_specs=[VMEM, VMEM, HBM],
        out_specs=(VMEM, VMEM, HBM),
        scratch_shapes=[
            pltpu.VMEM((rows, order), jnp.float32),
            pltpu.VMEM((6, order, order), jnp.bfloat16),
            pltpu.VMEM((order, order), jnp.float32),
            pltpu.VMEM((order, 2 * order), jnp.float32),
            pltpu.SemaphoreType.DMA((2,)),
        ],
        compiler_params=pltpu.CompilerParams(vmem_limit_bytes=VMEM_BYTES),
        cost_estimate=pl.CostEstimate(flops=18 * 10**9, bytes_accessed=6 * 4 * order**2, transcendentals=0),
    )(mine, other, in_hbm(panel))


def update_kernel(
    inv_rows, parts_hbm, head_mine, head_other, rest_mine, rest_other, trailing_ref,
    proj_hbm, updated_hbm, proj_ref, updated_ref, parts_ref, sent, arrived,
):
    first = lax.axis_index("core") == 0
    width = parts_ref.shape[1]
    loads = [
        pltpu.make_async_copy(parts_hbm.at[3 * i:3 * i + 3], parts_ref.at[3 * i:3 * i + 3], arrived.at[i])
        for i in range(2)
    ]
    for load in loads:
        load.start()
    count = trailing_ref.shape[1] // width
    areas = [slice(width * t, width * t + width) for t in range(count)]
    loads[0].wait()
    inverse = [parts_ref[i] for i in range(3)]
    stores = []

    def project(tile):
        if tile == 0:
            halves = ordered(first, head_mine[:, areas[1]], head_other[:, areas[1]])
        else:
            halves = ordered(first, rest_mine[:, areas[tile - 1]], rest_other[:, areas[tile - 1]])
        proj = matmul(inverse, thirds(jnp.concatenate(halves, axis=0) * inv_rows))
        proj_ref[:, areas[tile]] = proj
        return thirds(proj)

    def send(source, target, tile, slot):
        copy = pltpu.make_async_copy(source.at[:, areas[tile]], target.at[:, areas[tile]], sent.at[slot])
        copy.start()
        stores.append(copy)

    ahead = project(0)
    loads[1].wait()
    basis = [parts_ref[i + 3] for i in range(3)]
    for tile in range(count):
        proj = ahead
        if tile + 1 < count:
            ahead = project(tile + 1)
        updated_ref[:, areas[tile]] = trailing_ref[:, areas[tile]] - matmul(basis, proj)
        send(proj_ref, proj_hbm, tile, 2 * tile)
        send(updated_ref, updated_hbm, tile, 2 * tile + 1)
    for copy in stores:
        copy.wait()


def update(parts, grams, rest, trailing, inv_rows):
    width = parts.shape[1]
    rows, columns = trailing.shape
    shapes = ((width, columns), (rows, columns))
    return pl.pallas_call(
        functools.partial(update_kernel, inv_rows),
        out_shape=tuple(jax.ShapeDtypeStruct(shape, jnp.float32) for shape in shapes),
        in_specs=[HBM] + [VMEM] * 5,
        out_specs=(HBM, HBM),
        scratch_shapes=[
            *(pltpu.VMEM(shape, jnp.float32) for shape in shapes),
            pltpu.VMEM(parts.shape, parts.dtype),
            pltpu.SemaphoreType.DMA((2 * columns // width,)),
            pltpu.SemaphoreType.DMA((2,)),
        ],
        compiler_params=pltpu.CompilerParams(vmem_limit_bytes=VMEM_BYTES),
        cost_estimate=pl.CostEstimate(flops=24 * rows * width * columns, bytes_accessed=16 * rows * columns, transcendentals=0),
    )(in_hbm(parts), *grams, *rest, trailing)


def spread(block, axes):
    copies = jnp.broadcast_to(block[None], (lax.axis_size(axes),) + block.shape)
    return lax.all_to_all(copies, axes, 0, 0, tiled=True)


def swap_cores(value):
    return lax.ppermute(value, "core", ((0, 1), (1, 0)))


def per_device(panel, trailing):
    inv_rows = 1.0 / (panel.shape[0] * lax.axis_size(("y", "z", "core", "x")))
    width = panel.shape[1]
    half = width // 2
    columns = trailing.shape[1]
    plane = ("y", "x")
    mine, other = products(panel, trailing)
    mine = mine + swap_cores(other)
    pieces = mine.reshape(lax.axis_size(plane), -1, mine.shape[1])
    piece = jnp.sum(lax.all_to_all(pieces, plane, 0, 0, tiled=True), axis=0)
    row = jnp.sum(lax.all_to_all(piece, "z", 0, 0, tiled=True), axis=0)
    piece = spread(row, "z")
    first_part = jnp.concatenate([piece[:, :2 * width], piece[:, columns + width:]], axis=1)
    grams = spread(first_part, plane).reshape(half, -1)
    grams_other = swap_cores(grams)
    rest = spread(piece[:, 2 * width:columns + width], plane).reshape(half, -1)
    upper_panel, upper_next, parts = factor_two(grams, grams_other, panel, inv_rows)
    rest, upper_panel = lax.optimization_barrier((rest, upper_panel))
    projection, updated = update(
        parts, (grams, grams_other), (rest, swap_cores(rest)), trailing, inv_rows
    )
    return (upper_panel, projection, updated, upper_next)


def solution(mesh):
    chips = Mesh(mesh.devices.reshape(4, 8, 2, 4), ("y", "z", "core", "x"))
    rows = ("y", "z", "core", "x")
    return jax.shard_map(
        per_device,
        mesh=chips,
        in_specs=(P(rows, None), P(rows, None)),
        out_specs=(P(), P(), P(rows, None), P()),
        check_vma=False,
    )
```

```python
import functools
import itertools
import jax, jax.numpy as jnp
from jax import lax
from jax.experimental import pallas as pl
from jax.experimental.pallas import tpu as pltpu
from jax.sharding import Mesh, PartitionSpec as P

LANES = 128
VMEM_BYTES = 16 * 2**20
VMEM = pl.BlockSpec(memory_space=pltpu.VMEM)
HBM = pl.BlockSpec(memory_space=pltpu.HBM)


in_hbm = functools.partial(pltpu.with_memory_space_constraint, memory_space=pltpu.HBM)


def row_of(block, row):
    return jnp.broadcast_to(block[row:row + 1, :], block.shape)


def lane_of(block, lane):
    return jnp.broadcast_to(block[:, lane:lane + 1], block.shape)


def thirds(value):
    high = value.astype(jnp.bfloat16)
    rest = value - high.astype(jnp.float32)
    middle = rest.astype(jnp.bfloat16)
    low = (rest - middle.astype(jnp.float32)).astype(jnp.bfloat16)
    return high, middle, low


def matmul(left, right):
    l1, l2, l3 = left
    r1, r2, r3 = right
    pairs = ((l1, r3), (l3, r1), (l2, r2), (l1, r2), (l2, r1), (l1, r1))
    return sum(jnp.dot(a, b, preferred_element_type=jnp.float32) for a, b in pairs)


def outer(left, right):
    l1, l2, l3 = thirds(left)
    r1, r2, r3 = thirds(right)
    return lax.dot_general(
        jnp.concatenate([l1, l1, l2, l2, l1, l3], axis=0),
        jnp.concatenate([r1, r2, r1, r2, r3, r1], axis=0),
        (((0,), (0,)), ((), ())),
        preferred_element_type=jnp.float32,
    )


def factor(work, order, strip, extra, emit):
    groups = strip // 8
    sub_ids = lax.broadcasted_iota(jnp.int32, (8, LANES), 0)
    for start in range(0, order, strip):
        first = start // LANES
        stop = start + strip
        tiles = list(range(first, order // LANES))
        if extra:
            tiles += [order // LANES + t for t in range((stop + LANES - 1) // LANES)]
        rows = {
            (g, t): work[start + 8 * g:start + 8 * g + 8, LANES * t:LANES * t + LANES]
            for g in range(groups) for t in tiles
        }
        offset = start - LANES * first
        cols = {
            (m, g): lane_of(rows[g, first], offset + m)
            for m in range(strip) for g in range(m // 8, groups)
        }
        scale = [None] * groups
        for j in range(strip):
            g0, s0 = divmod(j, 8)
            inv_root = lax.rsqrt(row_of(cols[j, g0], s0))
            inv = inv_root * inv_root
            scale[g0] = inv_root if s0 == 0 else jnp.where(sub_ids == s0, inv_root, scale[g0])
            mult = {g: cols[j, g] * inv for g in range(g0, groups)}
            for m in range(j + 1, strip):
                entry = row_of(cols[j, m // 8], m % 8)
                for g in range(m // 8, groups):
                    cols[m, g] = cols[m, g] - mult[g] * entry
            if s0 == 7:
                del mult[g0]
            else:
                mult[g0] = jnp.where(sub_ids > s0, mult[g0], 0.0)
            for t in tiles:
                pivot_row = row_of(rows[g0, t], s0)
                for g in mult:
                    rows[g, t] = rows[g, t] - mult[g] * pivot_row
        for key in rows:
            rows[key] = rows[key] * scale[key[0]]
        block = {t: jnp.concatenate([rows[g, t] for g in range(groups)], axis=0) for t in tiles}
        emit(start, block)
        if stop == order:
            return
        base = stop // LANES
        left = jnp.concatenate([block[t] for t in range(base, order // LANES)], axis=1)
        keep = [t for t in tiles if t >= base]
        change = outer(left, jnp.concatenate([block[t] for t in keep], axis=1))
        for i, t in enumerate(keep):
            area = (slice(stop, order), slice(LANES * t, LANES * t + LANES))
            work[area] = work[area] - change[stop - LANES * base:, LANES * i:LANES * i + LANES]


def ordered(first, mine, other):
    return jnp.where(first, mine, other), jnp.where(first, other, mine)


def products_kernel(panel_hbm, trailing_hbm, mine_ref, other_ref, panel_ref, trailing_ref, arrived):
    first = lax.axis_index("core") == 0
    width = panel_ref.shape[1]
    half = width // 2
    count = trailing_ref.shape[1] // width
    areas = [slice(width * t, width * t + width) for t in range(count + 2)]
    loads = [pltpu.make_async_copy(panel_hbm, panel_ref, arrived.at[0])]
    for t in range(count):
        loads.append(pltpu.make_async_copy(
            trailing_hbm.at[:, areas[t]], trailing_ref.at[:, areas[t]], arrived.at[t + 1]
        ))
    for load in loads:
        load.start()
    loads[0].wait()
    panel = panel_ref[...]
    left_panel = thirds(panel.T)
    for tile in range(count + 2):
        left = left_panel
        if tile == 0:
            source = panel
        elif tile <= count:
            if tile == 1:
                for load in loads[1:]:
                    load.wait()
            source = trailing_ref[:, areas[tile - 1]]
        else:
            source = trailing_ref[:, areas[0]]
            left = thirds(source.T)
        result = matmul(left, thirds(source))
        mine_ref[:, areas[tile]], other_ref[:, areas[tile]] = ordered(first, result[:half], result[half:])


def products(panel, trailing):
    rows, width = panel.shape
    total = trailing.shape[1] + 2 * width
    shape = jax.ShapeDtypeStruct((width // 2, total), jnp.float32)
    return pl.pallas_call(
        products_kernel,
        out_shape=(shape, shape),
        in_specs=[HBM] * 2,
        out_specs=(VMEM,) * 2,
        scratch_shapes=[
            pltpu.VMEM(panel.shape, jnp.float32),
            pltpu.VMEM(trailing.shape, jnp.float32),
            pltpu.SemaphoreType.DMA((trailing.shape[1] // width + 1,)),
        ],
        compiler_params=pltpu.CompilerParams(vmem_limit_bytes=VMEM_BYTES),
        cost_estimate=pl.CostEstimate(flops=12 * rows * width * total, bytes_accessed=8 * rows * total, transcendentals=0),
    )(in_hbm(panel), in_hbm(trailing))


def pair_kernel(
    strip, inv_rows, mine_ref, other_ref, panel_hbm, upper_ref, next_ref, parts_hbm,
    panel_ref, parts_ref, inverse_ref, work, moved,
):
    load = pltpu.make_async_copy(panel_hbm, panel_ref, moved.at[0])
    load.start()
    store = pltpu.make_async_copy(parts_ref, parts_hbm, moved.at[1])
    order = upper_ref.shape[0]
    half = order // 2
    tiles = order // LANES
    first = lax.axis_index("core") == 0
    row_ids = lax.broadcasted_iota(jnp.int32, (order, order), 0)
    col_ids = lax.broadcasted_iota(jnp.int32, (order, order), 1)

    def block(index):
        area = slice(order * index, order * index + order)
        return jnp.concatenate(ordered(first, mine_ref[:, area], other_ref[:, area]), axis=0) * inv_rows

    work[:, :order] = block(0)
    work[:, order:] = jnp.where(row_ids == col_ids, 1.0, 0.0)
    upper_ref[...] = jnp.zeros_like(upper_ref)
    inverse_ref[...] = jnp.zeros_like(inverse_ref)
    next_ref[...] = jnp.zeros_like(next_ref)

    def emit_to(upper, inverse):
        def emit(start, block):
            ids = lax.broadcasted_iota(jnp.int32, (strip, LANES), 0) + start
            lanes = lax.broadcasted_iota(jnp.int32, (strip, LANES), 1)
            for t, value in block.items():
                if t < tiles:
                    value = jnp.where(lanes + LANES * t >= ids, value, 0.0)
                    upper[start:start + strip, LANES * t:LANES * t + LANES] = value
                else:
                    inverse[start:start + strip, LANES * (t - tiles):LANES * (t - tiles) + LANES] = value
        return emit

    factor(work, order, strip, True, emit_to(upper_ref, inverse_ref))
    inverse = thirds(inverse_ref[...])
    for index, part in enumerate(inverse):
        parts_ref[index] = part
    load.wait()
    basis = matmul(thirds(panel_ref[...]), thirds(inverse_ref[...].T))
    for index, part in enumerate(thirds(basis)):
        parts_ref[3 + index] = part
    store.start()
    proj = matmul(inverse, thirds(block(1)))
    work[:, :order] = block(2) - matmul(thirds(proj.T), thirds(proj))
    factor(work, order, strip, False, emit_to(next_ref, None))
    store.wait()


def factor_two(mine, other, panel, inv_rows, strip=16):
    rows, order = panel.shape
    shape = jax.ShapeDtypeStruct((order, order), jnp.float32)
    return pl.pallas_call(
        functools.partial(pair_kernel, strip, inv_rows),
        out_shape=(
            shape,
            shape,
            pltpu.HBM((6, order, order), jnp.bfloat16),
        ),
        in_specs=[VMEM, VMEM, HBM],
        out_specs=(VMEM, VMEM, HBM),
        scratch_shapes=[
            pltpu.VMEM((rows, order), jnp.float32),
            pltpu.VMEM((6, order, order), jnp.bfloat16),
            pltpu.VMEM((order, order), jnp.float32),
            pltpu.VMEM((order, 2 * order), jnp.float32),
            pltpu.SemaphoreType.DMA((2,)),
        ],
        compiler_params=pltpu.CompilerParams(vmem_limit_bytes=VMEM_BYTES),
        cost_estimate=pl.CostEstimate(flops=18 * 10**9, bytes_accessed=6 * 4 * order**2, transcendentals=0),
    )(mine, other, in_hbm(panel))


def update_kernel(
    inv_rows, parts_hbm, head_mine, head_other, rest_mine, rest_other, trailing_ref,
    proj_hbm, updated_hbm, proj_ref, updated_ref, parts_ref, sent, arrived,
):
    first = lax.axis_index("core") == 0
    width = parts_ref.shape[1]
    loads = [
        pltpu.make_async_copy(parts_hbm.at[3 * i:3 * i + 3], parts_ref.at[3 * i:3 * i + 3], arrived.at[i])
        for i in range(2)
    ]
    for load in loads:
        load.start()
    count = trailing_ref.shape[1] // width
    areas = [slice(width * t, width * t + width) for t in range(count)]
    loads[0].wait()
    inverse = [parts_ref[i] for i in range(3)]
    stores = []

    def project(tile):
        if tile == 0:
            halves = ordered(first, head_mine[:, areas[1]], head_other[:, areas[1]])
        else:
            halves = ordered(first, rest_mine[:, areas[tile - 1]], rest_other[:, areas[tile - 1]])
        proj = matmul(inverse, thirds(jnp.concatenate(halves, axis=0) * inv_rows))
        proj_ref[:, areas[tile]] = proj
        return thirds(proj)

    def send(source, target, tile, slot):
        copy = pltpu.make_async_copy(source.at[:, areas[tile]], target.at[:, areas[tile]], sent.at[slot])
        copy.start()
        stores.append(copy)

    ahead = project(0)
    loads[1].wait()
    basis = [parts_ref[i + 3] for i in range(3)]
    for tile in range(count):
        proj = ahead
        if tile + 1 < count:
            ahead = project(tile + 1)
        updated_ref[:, areas[tile]] = trailing_ref[:, areas[tile]] - matmul(basis, proj)
        send(proj_ref, proj_hbm, tile, 2 * tile)
        send(updated_ref, updated_hbm, tile, 2 * tile + 1)
    for copy in stores:
        copy.wait()


def update(parts, grams, rest, trailing, inv_rows):
    width = parts.shape[1]
    rows, columns = trailing.shape
    shapes = ((width, columns), (rows, columns))
    return pl.pallas_call(
        functools.partial(update_kernel, inv_rows),
        out_shape=tuple(jax.ShapeDtypeStruct(shape, jnp.float32) for shape in shapes),
        in_specs=[HBM] + [VMEM] * 5,
        out_specs=(HBM, HBM),
        scratch_shapes=[
            *(pltpu.VMEM(shape, jnp.float32) for shape in shapes),
            pltpu.VMEM(parts.shape, parts.dtype),
            pltpu.SemaphoreType.DMA((2 * columns // width,)),
            pltpu.SemaphoreType.DMA((2,)),
        ],
        compiler_params=pltpu.CompilerParams(vmem_limit_bytes=VMEM_BYTES),
        cost_estimate=pl.CostEstimate(flops=24 * rows * width * columns, bytes_accessed=16 * rows * columns, transcendentals=0),
    )(in_hbm(parts), *grams, *rest, trailing)


ROWS = ("y", "z", "core", "x")


def swap_cores(value):
    return lax.ppermute(value, "core", ((0, 1), (1, 0)))


def plane_shift(value, stage, step):
    pairs = []
    for y, z, core, x in itertools.product(range(4), range(8), range(2), range(4)):
        if core == stage:
            ny, nx = y, (x + step) % 4
        else:
            ny, nx = (y + step) % 4, x
        pairs.append((((y * 8 + z) * 2 + core) * 4 + x, ((ny * 8 + z) * 2 + core) * 4 + nx))
    return lax.ppermute(value, ROWS, pairs)


def plane_index(stage):
    return jnp.where(lax.axis_index("core") == stage, lax.axis_index("x"), lax.axis_index("y"))


def plane_sum(value, stage):
    chunks = value.reshape(4, value.shape[0] // 4, value.shape[1])
    index = plane_index(stage)
    total = lax.dynamic_index_in_dim(chunks, index, 0, keepdims=False)
    for step in range(1, 4):
        chunk = lax.dynamic_index_in_dim(chunks, (index + step) % 4, 0, keepdims=False)
        total = total + plane_shift(chunk, stage, step)
    return total


def plane_send(value, stage):
    return [value] + [plane_shift(value, stage, step) for step in range(1, 4)]


def plane_join(pieces, stage):
    rows, width = pieces[0].shape
    index = plane_index(stage)
    result = jnp.zeros((4 * rows, width), pieces[0].dtype)
    for step, piece in enumerate(pieces):
        result = lax.dynamic_update_slice(result, piece, ((index + 4 - step) % 4 * rows, 0))
    return result


def ring_sum(value):
    for bit in (1, 2, 4):
        value = value + lax.ppermute(value, "z", [(z, z ^ bit) for z in range(8)])
    return value


def per_device(panel, trailing):
    inv_rows = 1.0 / (panel.shape[0] * lax.axis_size(ROWS))
    width = panel.shape[1]
    columns = trailing.shape[1]
    mine, other = products(panel, trailing)
    mine = mine + swap_cores(other)
    piece = ring_sum(plane_sum(plane_sum(mine, 0), 1))
    piece = plane_join(plane_send(piece, 1), 1)
    first_part = jnp.concatenate([piece[:, :2 * width], piece[:, columns + width:]], axis=1)
    grams = plane_join(plane_send(first_part, 0), 0)
    grams_other = swap_cores(grams)
    rest_pieces = plane_send(piece[:, 2 * width:columns + width], 0)
    upper_panel, upper_next, parts = factor_two(grams, grams_other, panel, inv_rows)
    rest_pieces, upper_panel = lax.optimization_barrier((rest_pieces, upper_panel))
    rest = plane_join(rest_pieces, 0)
    projection, updated = update(
        parts, (grams, grams_other), (rest, swap_cores(rest)), trailing, inv_rows
    )
    return (upper_panel, projection, updated, upper_next)


def solution(mesh):
    chips = Mesh(mesh.devices.reshape(4, 8, 2, 4), ROWS)
    return jax.shard_map(
        per_device,
        mesh=chips,
        in_specs=(P(ROWS, None), P(ROWS, None)),
        out_specs=(P(), P(), P(ROWS, None), P()),
        check_vma=False,
    )
```

```python
import functools
import itertools
import jax, jax.numpy as jnp
from jax import lax
from jax.experimental import pallas as pl
from jax.experimental.pallas import tpu as pltpu
from jax.sharding import Mesh, PartitionSpec as P

LANES = 128
VMEM_BYTES = 16 * 2**20
VMEM = pl.BlockSpec(memory_space=pltpu.VMEM)
HBM = pl.BlockSpec(memory_space=pltpu.HBM)


in_hbm = functools.partial(pltpu.with_memory_space_constraint, memory_space=pltpu.HBM)
in_vmem = functools.partial(pltpu.with_memory_space_constraint, memory_space=pltpu.VMEM)


def row_of(block, row):
    return jnp.broadcast_to(block[row:row + 1, :], block.shape)


def lane_of(block, lane):
    return jnp.broadcast_to(block[:, lane:lane + 1], block.shape)


def thirds(value):
    high = value.astype(jnp.bfloat16)
    rest = value - high.astype(jnp.float32)
    middle = rest.astype(jnp.bfloat16)
    low = (rest - middle.astype(jnp.float32)).astype(jnp.bfloat16)
    return high, middle, low


def matmul(left, right):
    l1, l2, l3 = left
    r1, r2, r3 = right
    pairs = ((l1, r3), (l3, r1), (l2, r2), (l1, r2), (l2, r1), (l1, r1))
    return sum(jnp.dot(a, b, preferred_element_type=jnp.float32) for a, b in pairs)


def outer(left, right):
    l1, l2, l3 = thirds(left)
    r1, r2, r3 = thirds(right)
    return lax.dot_general(
        jnp.concatenate([l1, l1, l2, l2, l1, l3], axis=0),
        jnp.concatenate([r1, r2, r1, r2, r3, r1], axis=0),
        (((0,), (0,)), ((), ())),
        preferred_element_type=jnp.float32,
    )


def factor(work, order, strip, extra, emit):
    groups = strip // 8
    base_tiles = order // LANES
    sub_ids = lax.broadcasted_iota(jnp.int32, (8, LANES), 0)

    def tiles_of(start):
        tiles = list(range(start // LANES, base_tiles))
        if extra:
            tiles += [base_tiles + t for t in range((start + strip + LANES - 1) // LANES)]
        return tiles

    def load(start, group, tile):
        row = start + 8 * group
        return work[row:row + 8, LANES * tile:LANES * tile + LANES]

    rows = {(g, t): load(0, g, t) for g in range(groups) for t in tiles_of(0)}
    for start in range(0, order, strip):
        stop = start + strip
        first, offset = divmod(start, LANES)
        tiles = tiles_of(start)
        active = groups
        if stop < order:
            active = 2 * groups
            for g in range(groups):
                for t in {first, *tiles_of(stop)}:
                    rows[groups + g, t] = load(stop, g, t)
        cols = {
            (m, g): lane_of(rows[g, first], offset + m)
            for m in range(strip) for g in range(m // 8, active)
        }
        scale = [None] * groups
        for j in range(strip):
            g0, s0 = divmod(j, 8)
            inv_root = lax.rsqrt(row_of(cols[j, g0], s0))
            inv = inv_root * inv_root
            scale[g0] = inv_root if s0 == 0 else jnp.where(sub_ids == s0, inv_root, scale[g0])
            mult = {g: cols[j, g] * inv for g in range(g0, active)}
            for m in range(j + 1, strip):
                entry = row_of(cols[j, m // 8], m % 8)
                for g in range(m // 8, active):
                    cols[m, g] = cols[m, g] - mult[g] * entry
            if s0 == 7:
                del mult[g0]
            else:
                mult[g0] = jnp.where(sub_ids > s0, mult[g0], 0.0)
            for t in tiles:
                pivot_row = row_of(rows[g0, t], s0)
                for g in mult:
                    if (g, t) in rows:
                        rows[g, t] = rows[g, t] - mult[g] * pivot_row
        block = {
            t: jnp.concatenate([rows[g, t] * scale[g] for g in range(groups)], axis=0) for t in tiles
        }
        emit(start, block)
        rows = {(g - groups, t): value for (g, t), value in rows.items() if g >= groups}
        after = stop + strip
        if after >= order:
            continue
        base = after // LANES
        left = jnp.concatenate([block[t] for t in range(base, base_tiles)], axis=1)
        keep = [t for t in tiles if t >= stop // LANES]
        change = outer(left, jnp.concatenate([block[t] for t in keep], axis=1))
        for i, t in enumerate(keep):
            area = (slice(after, order), slice(LANES * t, LANES * t + LANES))
            work[area] = work[area] - change[after - LANES * base:, LANES * i:LANES * i + LANES]


def ordered(first, mine, other):
    return jnp.where(first, mine, other), jnp.where(first, other, mine)


def products_kernel(panel_hbm, trailing_hbm, mine_ref, other_ref, panel_ref, trailing_ref, arrived):
    first = lax.axis_index("core") == 0
    width = panel_ref.shape[1]
    half = width // 2
    count = trailing_ref.shape[1] // width
    areas = [slice(width * t, width * t + width) for t in range(count + 2)]
    loads = [pltpu.make_async_copy(panel_hbm, panel_ref, arrived.at[0])]
    for t in range(count):
        loads.append(pltpu.make_async_copy(
            trailing_hbm.at[:, areas[t]], trailing_ref.at[:, areas[t]], arrived.at[t + 1]
        ))
    for load in loads:
        load.start()
    loads[0].wait()
    panel = panel_ref[...]
    left_panel = thirds(panel.T)
    for tile in range(count + 2):
        left = left_panel
        if tile == 0:
            source = panel
        elif tile <= count:
            if tile == 1:
                for load in loads[1:]:
                    load.wait()
            source = trailing_ref[:, areas[tile - 1]]
        else:
            source = trailing_ref[:, areas[0]]
            left = thirds(source.T)
        result = matmul(left, thirds(source))
        mine_ref[:, areas[tile]], other_ref[:, areas[tile]] = ordered(first, result[:half], result[half:])


def products(panel, trailing):
    rows, width = panel.shape
    total = trailing.shape[1] + 2 * width
    shape = jax.ShapeDtypeStruct((width // 2, total), jnp.float32)
    return pl.pallas_call(
        products_kernel,
        out_shape=(shape, shape),
        in_specs=[HBM] * 2,
        out_specs=(VMEM,) * 2,
        scratch_shapes=[
            pltpu.VMEM(panel.shape, jnp.float32),
            pltpu.VMEM(trailing.shape, jnp.float32),
            pltpu.SemaphoreType.DMA((trailing.shape[1] // width + 1,)),
        ],
        compiler_params=pltpu.CompilerParams(vmem_limit_bytes=VMEM_BYTES),
        cost_estimate=pl.CostEstimate(flops=12 * rows * width * total, bytes_accessed=8 * rows * total, transcendentals=0),
    )(in_hbm(panel), in_hbm(trailing))


def emit_upper(upper, inverse, strip):
    tiles = upper.shape[0] // LANES

    def emit(start, block):
        ids = lax.broadcasted_iota(jnp.int32, (strip, LANES), 0) + start
        lanes = lax.broadcasted_iota(jnp.int32, (strip, LANES), 1)
        for t, value in block.items():
            if t < tiles:
                value = jnp.where(lanes + LANES * t >= ids, value, 0.0)
                upper[start:start + strip, LANES * t:LANES * t + LANES] = value
            else:
                inverse[start:start + strip, LANES * (t - tiles):LANES * (t - tiles) + LANES] = value
    return emit


def panel_kernel(
    strip, inv_rows, mine_ref, other_ref, panel_hbm, upper_ref, next_ref, parts_hbm,
    panel_ref, parts_ref, inverse_ref, work, moved,
):
    load = pltpu.make_async_copy(panel_hbm, panel_ref, moved.at[0])
    load.start()
    store = pltpu.make_async_copy(parts_ref, parts_hbm, moved.at[1])
    order = upper_ref.shape[0]
    first = lax.axis_index("core") == 0
    row_ids = lax.broadcasted_iota(jnp.int32, (order, order), 0)
    col_ids = lax.broadcasted_iota(jnp.int32, (order, order), 1)

    def block(index):
        area = slice(order * index, order * index + order)
        return jnp.concatenate(ordered(first, mine_ref[:, area], other_ref[:, area]), axis=0) * inv_rows

    work[:, :order] = block(0)
    work[:, order:] = jnp.where(row_ids == col_ids, 1.0, 0.0)
    upper_ref[...] = jnp.zeros_like(upper_ref)
    inverse_ref[...] = jnp.zeros_like(inverse_ref)
    factor(work, order, strip, True, emit_upper(upper_ref, inverse_ref, strip))
    inverse = thirds(inverse_ref[...])
    for index, part in enumerate(inverse):
        parts_ref[index] = part
    load.wait()
    proj = matmul(inverse, thirds(block(1)))
    basis = matmul(thirds(panel_ref[...]), thirds(inverse_ref[...].T))
    for index, part in enumerate(thirds(basis)):
        parts_ref[3 + index] = part
    next_ref[...] = block(2) - matmul(thirds(proj.T), thirds(proj))
    store.start()
    store.wait()


def next_kernel(strip, gram_ref, upper_ref, work):
    order = upper_ref.shape[0]
    work[...] = gram_ref[...]
    upper_ref[...] = jnp.zeros_like(upper_ref)
    factor(work, order, strip, False, emit_upper(upper_ref, None, strip))


def factor_panel(mine, other, panel, inv_rows, strip=16):
    rows, order = panel.shape
    shape = jax.ShapeDtypeStruct((order, order), jnp.float32)
    return pl.pallas_call(
        functools.partial(panel_kernel, strip, inv_rows),
        out_shape=(shape, shape, pltpu.HBM((6, order, order), jnp.bfloat16)),
        in_specs=[VMEM, VMEM, HBM],
        out_specs=(VMEM, VMEM, HBM),
        scratch_shapes=[
            pltpu.VMEM((rows, order), jnp.float32),
            pltpu.VMEM((6, order, order), jnp.bfloat16),
            pltpu.VMEM((order, order), jnp.float32),
            pltpu.VMEM((order, 2 * order), jnp.float32),
            pltpu.SemaphoreType.DMA((2,)),
        ],
        compiler_params=pltpu.CompilerParams(vmem_limit_bytes=VMEM_BYTES),
        cost_estimate=pl.CostEstimate(flops=9 * 10**9, bytes_accessed=6 * 4 * order**2, transcendentals=0),
    )(in_vmem(mine), in_vmem(other), in_hbm(panel))


def factor_next(gram, strip=16):
    order = gram.shape[0]
    return pl.pallas_call(
        functools.partial(next_kernel, strip),
        out_shape=jax.ShapeDtypeStruct((order, order), jnp.float32),
        in_specs=[VMEM],
        out_specs=VMEM,
        scratch_shapes=[pltpu.VMEM((order, order), jnp.float32)],
        compiler_params=pltpu.CompilerParams(vmem_limit_bytes=VMEM_BYTES),
        cost_estimate=pl.CostEstimate(flops=8 * 10**9, bytes_accessed=2 * 4 * order**2, transcendentals=0),
    )(gram)


def split_kernel(stage, mine_ref, arrived_ref, *chunk_refs):
    index = plane_index(stage)
    rows = chunk_refs[0].shape[0]
    for step, chunk_ref in enumerate(chunk_refs):
        area = pl.ds(lax.rem(index + step, 4) * rows, rows)
        chunk_ref[...] = mine_ref[area, :] + arrived_ref[area, :]


def add_split(mine, arrived, stage):
    rows, width = mine.shape
    return pl.pallas_call(
        functools.partial(split_kernel, stage),
        out_shape=(jax.ShapeDtypeStruct((rows // 4, width), jnp.float32),) * 4,
        in_specs=[VMEM] * 2,
        out_specs=(VMEM,) * 4,
        compiler_params=pltpu.CompilerParams(vmem_limit_bytes=VMEM_BYTES),
        cost_estimate=pl.CostEstimate(flops=10**8, bytes_accessed=12 * rows * width, transcendentals=0),
    )(in_vmem(mine), in_vmem(arrived))


def update_kernel(
    inv_rows, parts_ref, head_mine, head_other, rest_mine, rest_other, trailing_ref,
    proj_hbm, updated_hbm, proj_ref, updated_ref, sent,
):
    first = lax.axis_index("core") == 0
    width = parts_ref.shape[1]
    count = trailing_ref.shape[1] // width
    areas = [slice(width * t, width * t + width) for t in range(count)]
    inverse = [parts_ref[i] for i in range(3)]
    stores = []

    def project(tile):
        if tile == 0:
            halves = ordered(first, head_mine[:, areas[1]], head_other[:, areas[1]])
        else:
            halves = ordered(first, rest_mine[:, areas[tile - 1]], rest_other[:, areas[tile - 1]])
        proj = matmul(inverse, thirds(jnp.concatenate(halves, axis=0) * inv_rows))
        proj_ref[:, areas[tile]] = proj
        return thirds(proj)

    def send(source, target, tile, slot):
        copy = pltpu.make_async_copy(source.at[:, areas[tile]], target.at[:, areas[tile]], sent.at[slot])
        copy.start()
        stores.append(copy)

    ahead = project(0)
    basis = [parts_ref[i + 3] for i in range(3)]
    for tile in range(count):
        proj = ahead
        if tile + 1 < count:
            ahead = project(tile + 1)
        updated_ref[:, areas[tile]] = trailing_ref[:, areas[tile]] - matmul(basis, proj)
        send(proj_ref, proj_hbm, tile, 2 * tile)
        send(updated_ref, updated_hbm, tile, 2 * tile + 1)
    for copy in stores:
        copy.wait()


def update(parts, grams, rest, trailing, inv_rows):
    width = parts.shape[1]
    rows, columns = trailing.shape
    shapes = ((width, columns), (rows, columns))
    return pl.pallas_call(
        functools.partial(update_kernel, inv_rows),
        out_shape=tuple(jax.ShapeDtypeStruct(shape, jnp.float32) for shape in shapes),
        in_specs=[VMEM] * 6,
        out_specs=(HBM, HBM),
        scratch_shapes=[
            *(pltpu.VMEM(shape, jnp.float32) for shape in shapes),
            pltpu.SemaphoreType.DMA((2 * columns // width,)),
        ],
        compiler_params=pltpu.CompilerParams(vmem_limit_bytes=VMEM_BYTES),
        cost_estimate=pl.CostEstimate(flops=24 * rows * width * columns, bytes_accessed=16 * rows * columns, transcendentals=0),
    )(parts, *grams, *rest, trailing)


ROWS = ("y", "z", "core", "x")


def swap_cores(value):
    return lax.ppermute(value, "core", ((0, 1), (1, 0)))


def plane_shift(value, stage, step):
    pairs = []
    for y, z, core, x in itertools.product(range(4), range(8), range(2), range(4)):
        if core == stage:
            ny, nx = y, (x + step) % 4
        else:
            ny, nx = (y + step) % 4, x
        pairs.append((((y * 8 + z) * 2 + core) * 4 + x, ((ny * 8 + z) * 2 + core) * 4 + nx))
    return lax.ppermute(value, ROWS, pairs)


def plane_index(stage):
    return jnp.where(lax.axis_index("core") == stage, lax.axis_index("x"), lax.axis_index("y"))


def plane_sum(chunks, stage):
    total = chunks[0]
    for step in range(1, 4):
        total = total + plane_shift(chunks[step], stage, step)
    return total


def plane_chunks(value, stage):
    chunks = value.reshape(4, value.shape[0] // 4, value.shape[1])
    index = plane_index(stage)
    return [
        lax.dynamic_index_in_dim(chunks, (index + step) % 4, 0, keepdims=False) for step in range(4)
    ]


def plane_send(value, stage):
    return [value] + [plane_shift(value, stage, step) for step in range(1, 4)]


def plane_join(pieces, stage):
    rows, width = pieces[0].shape
    index = plane_index(stage)
    result = jnp.zeros((4 * rows, width), pieces[0].dtype)
    for step, piece in enumerate(pieces):
        result = lax.dynamic_update_slice(result, piece, ((index + 4 - step) % 4 * rows, 0))
    return result


def ring_sum(value):
    for bit in (1, 2, 4):
        value = value + lax.ppermute(value, "z", [(z, z ^ bit) for z in range(8)])
    return value


def per_device(panel, trailing):
    inv_rows = 1.0 / (panel.shape[0] * lax.axis_size(ROWS))
    width = panel.shape[1]
    columns = trailing.shape[1]
    mine, other = products(panel, trailing)
    piece = plane_sum(add_split(mine, swap_cores(other), 0), 0)
    piece = ring_sum(plane_sum(plane_chunks(piece, 1), 1))
    piece = plane_join(plane_send(piece, 1), 1)
    first_part = jnp.concatenate([piece[:, :2 * width], piece[:, columns + width:]], axis=1)
    grams = plane_join(plane_send(first_part, 0), 0)
    grams_other = swap_cores(grams)
    rest_pieces = plane_send(piece[:, 2 * width:columns + width], 0)
    upper_panel, gram_next, parts = factor_panel(grams, grams_other, panel, inv_rows)
    rest_pieces, gram_next = lax.optimization_barrier((rest_pieces, gram_next))
    rest = plane_join(rest_pieces, 0)
    rest, gram_next = lax.optimization_barrier((rest, gram_next))
    rest_other = swap_cores(rest)
    upper_next = factor_next(gram_next)
    projection, updated = update(parts, (grams, grams_other), (rest, rest_other), trailing, inv_rows)
    return (upper_panel, projection, updated, upper_next)


def solution(mesh):
    chips = Mesh(mesh.devices.reshape(4, 8, 2, 4), ROWS)
    return jax.shard_map(
        per_device,
        mesh=chips,
        in_specs=(P(ROWS, None), P(ROWS, None)),
        out_specs=(P(), P(), P(ROWS, None), P()),
        check_vma=False,
    )
```

```python
import functools
import itertools
import jax, jax.numpy as jnp
from jax import lax
from jax.experimental import pallas as pl
from jax.experimental.pallas import tpu as pltpu
from jax.sharding import Mesh, PartitionSpec as P


LANES = 128
VMEM_BYTES = 16 * 2**20
VMEM = pl.BlockSpec(memory_space=pltpu.VMEM)
HBM = pl.BlockSpec(memory_space=pltpu.HBM)


in_hbm = functools.partial(pltpu.with_memory_space_constraint, memory_space=pltpu.HBM)
in_vmem = functools.partial(pltpu.with_memory_space_constraint, memory_space=pltpu.VMEM)


def row_of(block, row):
    return jnp.broadcast_to(block[row:row + 1, :], block.shape)


def lane_of(block, lane):
    return jnp.broadcast_to(block[:, lane:lane + 1], block.shape)


def thirds(value):
    high = value.astype(jnp.bfloat16)
    rest = value - high.astype(jnp.float32)
    middle = rest.astype(jnp.bfloat16)
    low = (rest - middle.astype(jnp.float32)).astype(jnp.bfloat16)
    return high, middle, low


def matmul(left, right):
    l1, l2, l3 = left
    r1, r2, r3 = right
    pairs = ((l1, r3), (l3, r1), (l2, r2), (l1, r2), (l2, r1), (l1, r1))
    return sum(jnp.dot(a, b, preferred_element_type=jnp.float32) for a, b in pairs)


def outer(left, right):
    l1, l2, l3 = thirds(left)
    r1, r2, r3 = thirds(right)
    return lax.dot_general(
        jnp.concatenate([l1, l1, l2, l2, l1, l3], axis=0),
        jnp.concatenate([r1, r2, r1, r2, r3, r1], axis=0),
        (((0,), (0,)), ((), ())),
        preferred_element_type=jnp.float32,
    )


def factor(work, order, strip, extra, emit):
    groups = strip // 8
    base_tiles = order // LANES
    sub_ids = lax.broadcasted_iota(jnp.int32, (8, LANES), 0)

    def tiles_of(start):
        tiles = list(range(start // LANES, base_tiles))
        if extra:
            tiles += [base_tiles + t for t in range((start + strip + LANES - 1) // LANES)]
        return tiles

    def load(start, group, tile):
        row = start + 8 * group
        return work[row:row + 8, LANES * tile:LANES * tile + LANES]

    rows = {(g, t): load(0, g, t) for g in range(groups) for t in tiles_of(0)}
    for start in range(0, order, strip):
        stop = start + strip
        first, offset = divmod(start, LANES)
        tiles = tiles_of(start)
        active = groups
        if stop < order:
            active = 2 * groups
            for g in range(groups):
                for t in {first, *tiles_of(stop)}:
                    rows[groups + g, t] = load(stop, g, t)
        cols = {
            (m, g): lane_of(rows[g, first], offset + m)
            for m in range(strip) for g in range(m // 8, active)
        }
        scale = [None] * groups
        for j in range(strip):
            g0, s0 = divmod(j, 8)
            inv_root = lax.rsqrt(row_of(cols[j, g0], s0))
            inv = inv_root * inv_root
            scale[g0] = inv_root if s0 == 0 else jnp.where(sub_ids == s0, inv_root, scale[g0])
            mult = {g: cols[j, g] * inv for g in range(g0, active)}
            for m in range(j + 1, strip):
                entry = row_of(cols[j, m // 8], m % 8)
                for g in range(m // 8, active):
                    cols[m, g] = cols[m, g] - mult[g] * entry
            if s0 == 7:
                del mult[g0]
            else:
                mult[g0] = jnp.where(sub_ids > s0, mult[g0], 0.0)
            for t in tiles:
                pivot_row = row_of(rows[g0, t], s0)
                for g in mult:
                    if (g, t) in rows:
                        rows[g, t] = rows[g, t] - mult[g] * pivot_row
        block = {
            t: jnp.concatenate([rows[g, t] * scale[g] for g in range(groups)], axis=0) for t in tiles
        }
        emit(start, block)
        rows = {(g - groups, t): value for (g, t), value in rows.items() if g >= groups}
        after = stop + strip
        if after >= order:
            continue
        base = after // LANES
        left = jnp.concatenate([block[t] for t in range(base, base_tiles)], axis=1)
        keep = [t for t in tiles if t >= stop // LANES]
        change = outer(left, jnp.concatenate([block[t] for t in keep], axis=1))
        for i, t in enumerate(keep):
            area = (slice(after, order), slice(LANES * t, LANES * t + LANES))
            work[area] = work[area] - change[after - LANES * base:, LANES * i:LANES * i + LANES]


def ordered(first, mine, other):
    return jnp.where(first, mine, other), jnp.where(first, other, mine)


def products_kernel(
    panel_hbm, trailing_hbm, gram_mine, gram_other, rest_mine, rest_other, panel_ref, trailing_ref, arrived,
):
    first = lax.axis_index("core") == 0
    width = panel_ref.shape[1]
    half = width // 2
    count = trailing_ref.shape[1] // width
    areas = [slice(width * t, width * t + width) for t in range(count)]
    loads = [
        pltpu.make_async_copy(panel_hbm, panel_ref, arrived.at[0]),
        pltpu.make_async_copy(trailing_hbm.at[:, areas[0]], trailing_ref.at[:, areas[0]], arrived.at[1]),
        pltpu.make_async_copy(trailing_hbm.at[:, width:], trailing_ref.at[:, width:], arrived.at[2]),
    ]
    for load in loads:
        load.start()

    def put(mine_ref, other_ref, tile, left, source):
        result = matmul(left, thirds(source))
        mine_ref[:, areas[tile]], other_ref[:, areas[tile]] = ordered(first, result[:half], result[half:])

    loads[0].wait()
    loads[1].wait()
    panel = panel_ref[...]
    head = trailing_ref[:, areas[0]]
    left = thirds(panel.T)
    put(gram_mine, gram_other, 0, left, panel)
    put(gram_mine, gram_other, 1, left, head)
    put(gram_mine, gram_other, 2, thirds(head.T), head)
    loads[2].wait()
    for tile in range(1, count):
        put(rest_mine, rest_other, tile - 1, left, trailing_ref[:, areas[tile]])


def products(panel, trailing):
    rows, width = panel.shape
    columns = trailing.shape[1]
    grams = jax.ShapeDtypeStruct((width // 2, 3 * width), jnp.float32)
    rest = jax.ShapeDtypeStruct((width // 2, columns - width), jnp.float32)
    total = columns + 2 * width
    return pl.pallas_call(
        products_kernel,
        out_shape=(grams, grams, rest, rest),
        in_specs=[HBM] * 2,
        out_specs=(VMEM,) * 4,
        scratch_shapes=[
            pltpu.VMEM(panel.shape, jnp.float32),
            pltpu.VMEM(trailing.shape, jnp.float32),
            pltpu.SemaphoreType.DMA((3,)),
        ],
        compiler_params=pltpu.CompilerParams(vmem_limit_bytes=VMEM_BYTES),
        cost_estimate=pl.CostEstimate(flops=12 * rows * width * total, bytes_accessed=8 * rows * total, transcendentals=0),
    )(in_hbm(panel), in_hbm(trailing))


def emit_upper(upper, inverse, strip):
    tiles = upper.shape[0] // LANES

    def emit(start, block):
        ids = lax.broadcasted_iota(jnp.int32, (strip, LANES), 0) + start
        lanes = lax.broadcasted_iota(jnp.int32, (strip, LANES), 1)
        for t, value in block.items():
            if t < tiles:
                value = jnp.where(lanes + LANES * t >= ids, value, 0.0)
                upper[start:start + strip, LANES * t:LANES * t + LANES] = value
            else:
                inverse[start:start + strip, LANES * (t - tiles):LANES * (t - tiles) + LANES] = value

    return emit


def panel_kernel(
    strip, inv_rows, mine_ref, other_ref, panel_hbm, upper_ref, next_ref, parts_hbm,
    panel_ref, parts_ref, inverse_ref, work, moved,
):
    load = pltpu.make_async_copy(panel_hbm, panel_ref, moved.at[0])
    load.start()
    store = pltpu.make_async_copy(parts_ref, parts_hbm, moved.at[1])
    order = upper_ref.shape[0]
    first = lax.axis_index("core") == 0
    row_ids = lax.broadcasted_iota(jnp.int32, (order, order), 0)
    col_ids = lax.broadcasted_iota(jnp.int32, (order, order), 1)

    def block(index):
        area = slice(order * index, order * index + order)
        return jnp.concatenate(ordered(first, mine_ref[:, area], other_ref[:, area]), axis=0) * inv_rows

    work[:, :order] = block(0)
    work[:, order:] = jnp.where(row_ids == col_ids, 1.0, 0.0)
    upper_ref[...] = jnp.zeros_like(upper_ref)
    inverse_ref[...] = jnp.zeros_like(inverse_ref)
    factor(work, order, strip, True, emit_upper(upper_ref, inverse_ref, strip))
    inverse = thirds(inverse_ref[...])
    for index, part in enumerate(inverse):
        parts_ref[index] = part
    load.wait()
    proj = matmul(inverse, thirds(block(1)))
    basis = matmul(thirds(panel_ref[...]), thirds(inverse_ref[...].T))
    for index, part in enumerate(thirds(basis)):
        parts_ref[3 + index] = part
    next_ref[...] = block(2) - matmul(thirds(proj.T), thirds(proj))
    store.start()
    store.wait()


def next_kernel(strip, gram_ref, upper_ref, work):
    order = upper_ref.shape[0]
    work[...] = gram_ref[...]
    upper_ref[...] = jnp.zeros_like(upper_ref)
    factor(work, order, strip, False, emit_upper(upper_ref, None, strip))


def factor_panel(mine, other, panel, inv_rows, strip=16):
    rows, order = panel.shape
    shape = jax.ShapeDtypeStruct((order, order), jnp.float32)
    return pl.pallas_call(
        functools.partial(panel_kernel, strip, inv_rows),
        out_shape=(shape, shape, pltpu.HBM((6, order, order), jnp.bfloat16)),
        in_specs=[VMEM, VMEM, HBM],
        out_specs=(VMEM, VMEM, HBM),
        scratch_shapes=[
            pltpu.VMEM((rows, order), jnp.float32),
            pltpu.VMEM((6, order, order), jnp.bfloat16),
            pltpu.VMEM((order, order), jnp.float32),
            pltpu.VMEM((order, 2 * order), jnp.float32),
            pltpu.SemaphoreType.DMA((2,)),
        ],
        compiler_params=pltpu.CompilerParams(vmem_limit_bytes=VMEM_BYTES),
        cost_estimate=pl.CostEstimate(flops=9 * 10**9, bytes_accessed=6 * 4 * order**2, transcendentals=0),
    )(in_vmem(mine), in_vmem(other), in_hbm(panel))


def factor_next(gram, strip=16):
    order = gram.shape[0]
    return pl.pallas_call(
        functools.partial(next_kernel, strip),
        out_shape=jax.ShapeDtypeStruct((order, order), jnp.float32),
        in_specs=[VMEM],
        out_specs=VMEM,
        scratch_shapes=[pltpu.VMEM((order, order), jnp.float32)],
        compiler_params=pltpu.CompilerParams(vmem_limit_bytes=VMEM_BYTES),
        cost_estimate=pl.CostEstimate(flops=8 * 10**9, bytes_accessed=2 * 4 * order**2, transcendentals=0),
    )(gram)


def split_kernel(stage, mine_ref, arrived_ref, *chunk_refs):
    index = plane_index(stage)
    rows = chunk_refs[0].shape[0]
    for step, chunk_ref in enumerate(chunk_refs):
        area = pl.ds(lax.rem(index + step, 4) * rows, rows)
        chunk_ref[...] = mine_ref[area, :] + arrived_ref[area, :]


def add_split(mine, arrived, stage):
    rows, width = mine.shape
    return pl.pallas_call(
        functools.partial(split_kernel, stage),
        out_shape=(jax.ShapeDtypeStruct((rows // 4, width), jnp.float32),) * 4,
        in_specs=[VMEM] * 2,
        out_specs=(VMEM,) * 4,
        compiler_params=pltpu.CompilerParams(vmem_limit_bytes=VMEM_BYTES),
        cost_estimate=pl.CostEstimate(flops=10**8, bytes_accessed=12 * rows * width, transcendentals=0),
    )(in_vmem(mine), in_vmem(arrived))


def update_kernel(
    inv_rows, parts_ref, head_mine, head_other, rest_mine, rest_other, trailing_ref,
    proj_hbm, updated_hbm, proj_ref, updated_ref, sent,
):
    first = lax.axis_index("core") == 0
    width = parts_ref.shape[1]
    count = trailing_ref.shape[1] // width
    areas = [slice(width * t, width * t + width) for t in range(count)]
    inverse = [parts_ref[i] for i in range(3)]
    stores = []

    def project(tile):
        if tile == 0:
            halves = ordered(first, head_mine[:, areas[1]], head_other[:, areas[1]])
        else:
            halves = ordered(first, rest_mine[:, areas[tile - 1]], rest_other[:, areas[tile - 1]])
        proj = matmul(inverse, thirds(jnp.concatenate(halves, axis=0) * inv_rows))
        proj_ref[:, areas[tile]] = proj
        return thirds(proj)

    def send(source, target, tile, slot):
        copy = pltpu.make_async_copy(source.at[:, areas[tile]], target.at[:, areas[tile]], sent.at[slot])
        copy.start()
        stores.append(copy)

    ahead = project(0)
    basis = [parts_ref[i + 3] for i in range(3)]
    for tile in range(count):
        proj = ahead
        if tile + 1 < count:
            ahead = project(tile + 1)
        updated_ref[:, areas[tile]] = trailing_ref[:, areas[tile]] - matmul(basis, proj)
        send(proj_ref, proj_hbm, tile, 2 * tile)
        send(updated_ref, updated_hbm, tile, 2 * tile + 1)
    for copy in stores:
        copy.wait()


def update(parts, grams, rest, trailing, inv_rows):
    width = parts.shape[1]
    rows, columns = trailing.shape
    shapes = ((width, columns), (rows, columns))
    return pl.pallas_call(
        functools.partial(update_kernel, inv_rows),
        out_shape=tuple(jax.ShapeDtypeStruct(shape, jnp.float32) for shape in shapes),
        in_specs=[VMEM] * 6,
        out_specs=(HBM, HBM),
        scratch_shapes=[
            *(pltpu.VMEM(shape, jnp.float32) for shape in shapes),
            pltpu.SemaphoreType.DMA((2 * columns // width,)),
        ],
        compiler_params=pltpu.CompilerParams(vmem_limit_bytes=VMEM_BYTES),
        cost_estimate=pl.CostEstimate(flops=24 * rows * width * columns, bytes_accessed=16 * rows * columns, transcendentals=0),
    )(parts, *grams, *rest, trailing)


ROWS = ("y", "z", "core", "x")


def swap_cores(value):
    return lax.ppermute(value, "core", ((0, 1), (1, 0)))


def plane_shift(value, stage, step):
    pairs = []
    for y, z, core, x in itertools.product(range(4), range(8), range(2), range(4)):
        if core == stage:
            ny, nx = y, (x + step) % 4
        else:
            ny, nx = (y + step) % 4, x
        pairs.append((((y * 8 + z) * 2 + core) * 4 + x, ((ny * 8 + z) * 2 + core) * 4 + nx))
    return lax.ppermute(value, ROWS, pairs)


def plane_index(stage):
    return jnp.where(lax.axis_index("core") == stage, lax.axis_index("x"), lax.axis_index("y"))


def plane_sum(chunks, stage):
    total = chunks[0]
    for step in range(1, 4):
        total = total + plane_shift(chunks[step], stage, step)
    return total


def plane_swap(value, stage, bit):
    pairs = []
    for y, z, core, x in itertools.product(range(4), range(8), range(2), range(4)):
        ny, nx = (y, x ^ bit) if core == stage else (y ^ bit, x)
        pairs.append((((y * 8 + z) * 2 + core) * 4 + x, ((ny * 8 + z) * 2 + core) * 4 + nx))
    return lax.ppermute(value, ROWS, pairs)


def halve(value, stage, bit):
    halves = value.reshape(2, value.shape[0] // 2, value.shape[1])
    side = plane_index(stage) // bit % 2
    mine = lax.dynamic_index_in_dim(halves, side, 0, keepdims=False)
    other = lax.dynamic_index_in_dim(halves, 1 - side, 0, keepdims=False)
    return mine + plane_swap(other, stage, bit)


def double(value, stage, bit):
    lower = plane_index(stage) // bit % 2 == 0
    return jnp.concatenate(ordered(lower, value, plane_swap(value, stage, bit)), axis=0)


def plane_send(value, stage):
    return [value] + [plane_shift(value, stage, step) for step in range(1, 4)]


def plane_join(pieces, stage):
    rows, width = pieces[0].shape
    index = plane_index(stage)
    result = jnp.zeros((4 * rows, width), pieces[0].dtype)
    for step, piece in enumerate(pieces):
        result = lax.dynamic_update_slice(result, piece, ((index + 4 - step) % 4 * rows, 0))
    return result


def partner_sum(value, bit):
    return value + lax.ppermute(value, "z", [(z, z ^ bit) for z in range(8)])


def per_device(panel, trailing):
    inv_rows = 1.0 / (panel.shape[0] * lax.axis_size(ROWS))
    gram_mine, gram_other, rest_mine, rest_other = products(panel, trailing)
    stages = (
        lambda v: add_split(v[0], swap_cores(v[1]), 0),
        lambda v: plane_sum(v, 0),
        lambda v: halve(v, 1, 2),
        lambda v: halve(v, 1, 1),
        lambda v: partner_sum(v, 1),
        lambda v: partner_sum(v, 2),
        lambda v: partner_sum(v, 4),
        lambda v: double(v, 1, 1),
        lambda v: double(v, 1, 2),
        lambda v: plane_send(v, 0),
    )
    lead, lag = (gram_mine, gram_other), (rest_mine, rest_other)
    for stage in stages:
        lead = stage(lead)
        lag = stage(lag)
    grams = plane_join(lead, 0)
    grams_other = swap_cores(grams)
    rest_pieces = lag
    upper_panel, gram_next, parts = factor_panel(grams, grams_other, panel, inv_rows)
    rest_pieces, gram_next = lax.optimization_barrier((rest_pieces, gram_next))
    rest = plane_join(rest_pieces, 0)
    rest, gram_next = lax.optimization_barrier((rest, gram_next))
    rest_other = swap_cores(rest)
    upper_next = factor_next(gram_next)
    projection, updated = update(parts, (grams, grams_other), (rest, rest_other), trailing, inv_rows)
    return (upper_panel, projection, updated, upper_next)


def solution(mesh):
    chips = Mesh(mesh.devices.reshape(4, 8, 2, 4), ROWS)

    return jax.shard_map(
        per_device,
        mesh=chips,
        in_specs=(P(ROWS, None), P(ROWS, None)),
        out_specs=(P(), P(), P(ROWS, None), P()),
        check_vma=False,
    )
```

```python
import functools
import itertools
import jax, jax.numpy as jnp
from jax import lax
from jax.experimental import pallas as pl
from jax.experimental.pallas import tpu as pltpu
from jax.sharding import Mesh, PartitionSpec as P

LANES = 128
VMEM_BYTES = 16 * 2**20
VMEM = pl.BlockSpec(memory_space=pltpu.VMEM)
HBM = pl.BlockSpec(memory_space=pltpu.HBM)


in_hbm = functools.partial(pltpu.with_memory_space_constraint, memory_space=pltpu.HBM)
in_vmem = functools.partial(pltpu.with_memory_space_constraint, memory_space=pltpu.VMEM)


def row_of(block, row):
    return jnp.broadcast_to(block[row:row + 1, :], block.shape)


def lane_of(block, lane):
    return jnp.broadcast_to(block[:, lane:lane + 1], block.shape)


def thirds(value):
    high = value.astype(jnp.bfloat16)
    rest = value - high.astype(jnp.float32)
    middle = rest.astype(jnp.bfloat16)
    low = (rest - middle.astype(jnp.float32)).astype(jnp.bfloat16)
    return high, middle, low


def matmul(left, right):
    l1, l2, l3 = left
    r1, r2, r3 = right
    pairs = ((l1, r3), (l3, r1), (l2, r2), (l1, r2), (l2, r1), (l1, r1))
    return sum(jnp.dot(a, b, preferred_element_type=jnp.float32) for a, b in pairs)


def outer(left, right):
    l1, l2, l3 = thirds(left)
    r1, r2, r3 = thirds(right)
    return lax.dot_general(
        jnp.concatenate([l1, l1, l2, l2, l1, l3], axis=0),
        jnp.concatenate([r1, r2, r1, r2, r3, r1], axis=0),
        (((0,), (0,)), ((), ())),
        preferred_element_type=jnp.float32,
    )


def factor(work, order, strip, extra, emit):
    groups = strip // 8
    base_tiles = order // LANES
    sub_ids = lax.broadcasted_iota(jnp.int32, (8, LANES), 0)

    def tiles_of(start):
        tiles = list(range(start // LANES, base_tiles))
        if extra:
            tiles += [base_tiles + t for t in range((start + strip + LANES - 1) // LANES)]
        return tiles

    def load(start, group, tile):
        row = start + 8 * group
        return work[row:row + 8, LANES * tile:LANES * tile + LANES]

    rows = {(g, t): load(0, g, t) for g in range(groups) for t in tiles_of(0)}
    for start in range(0, order, strip):
        stop = start + strip
        first, offset = divmod(start, LANES)
        tiles = tiles_of(start)
        active = groups
        if stop < order:
            active = 2 * groups
            for g in range(groups):
                for t in {first, *tiles_of(stop)}:
                    rows[groups + g, t] = load(stop, g, t)
        cols = {
            (m, g): lane_of(rows[g, first], offset + m)
            for m in range(strip) for g in range(m // 8, active)
        }
        scale = [None] * groups
        for j in range(strip):
            g0, s0 = divmod(j, 8)
            inv_root = lax.rsqrt(row_of(cols[j, g0], s0))
            inv = inv_root * inv_root
            scale[g0] = inv_root if s0 == 0 else jnp.where(sub_ids == s0, inv_root, scale[g0])
            mult = {g: cols[j, g] * inv for g in range(g0, active)}
            for m in range(j + 1, strip):
                entry = row_of(cols[j, m // 8], m % 8)
                for g in range(m // 8, active):
                    cols[m, g] = cols[m, g] - mult[g] * entry
            if s0 == 7:
                del mult[g0]
            else:
                mult[g0] = jnp.where(sub_ids > s0, mult[g0], 0.0)
            for t in tiles:
                pivot_row = row_of(rows[g0, t], s0)
                for g in mult:
                    if (g, t) in rows:
                        rows[g, t] = rows[g, t] - mult[g] * pivot_row
        block = {
            t: jnp.concatenate([rows[g, t] * scale[g] for g in range(groups)], axis=0) for t in tiles
        }
        emit(start, block)
        rows = {(g - groups, t): value for (g, t), value in rows.items() if g >= groups}
        after = stop + strip
        if after >= order:
            continue
        base = after // LANES
        left = jnp.concatenate([block[t] for t in range(base, base_tiles)], axis=1)
        keep = [t for t in tiles if t >= stop // LANES]
        change = outer(left, jnp.concatenate([block[t] for t in keep], axis=1))
        for i, t in enumerate(keep):
            area = (slice(after, order), slice(LANES * t, LANES * t + LANES))
            work[area] = work[area] - change[after - LANES * base:, LANES * i:LANES * i + LANES]


def ordered(first, mine, other):
    return jnp.where(first, mine, other), jnp.where(first, other, mine)


def products_kernel(
    lo, hi, panel_hbm, trailing_hbm, mine_ref, other_ref, panel_ref, trailing_ref, arrived,
):
    first = lax.axis_index("core") == 0
    width = panel_ref.shape[1]
    half = width // 2
    load_panel = pltpu.make_async_copy(panel_hbm, panel_ref, arrived.at[0])
    load_trailing = pltpu.make_async_copy(
        trailing_hbm.at[:, width * lo:width * hi], trailing_ref, arrived.at[1]
    )
    load_panel.start()
    load_trailing.start()
    load_panel.wait()
    panel = panel_ref[...]
    left = thirds(panel.T)
    slot = 0

    def put(slot, left, source):
        area = slice(width * slot, width * slot + width)
        result = matmul(left, thirds(source))
        mine_ref[:, area], other_ref[:, area] = ordered(first, result[:half], result[half:])

    if lo == 0:
        put(0, left, panel)
        slot = 1
    load_trailing.wait()
    for tile in range(hi - lo):
        source = trailing_ref[:, width * tile:width * tile + width]
        put(slot, left, source)
        slot += 1
        if lo + tile == 0:
            put(slot, thirds(source.T), source)
            slot += 1


def products(panel, trailing, lo, hi):
    rows, width = panel.shape
    total = (hi - lo + (2 if lo == 0 else 0)) * width
    shape = jax.ShapeDtypeStruct((width // 2, total), jnp.float32)
    return pl.pallas_call(
        functools.partial(products_kernel, lo, hi),
        out_shape=(shape, shape),
        in_specs=[HBM] * 2,
        out_specs=(VMEM,) * 2,
        scratch_shapes=[
            pltpu.VMEM(panel.shape, jnp.float32),
            pltpu.VMEM((rows, (hi - lo) * width), jnp.float32),
            pltpu.SemaphoreType.DMA((2,)),
        ],
        compiler_params=pltpu.CompilerParams(vmem_limit_bytes=VMEM_BYTES),
        cost_estimate=pl.CostEstimate(flops=2 * 10**9, bytes_accessed=8 * rows * total, transcendentals=0),
    )(in_hbm(panel), in_hbm(trailing))


def emit_upper(upper, inverse, strip):
    tiles = upper.shape[0] // LANES

    def emit(start, block):
        ids = lax.broadcasted_iota(jnp.int32, (strip, LANES), 0) + start
        lanes = lax.broadcasted_iota(jnp.int32, (strip, LANES), 1)
        for t, value in block.items():
            if t < tiles:
                value = jnp.where(lanes + LANES * t >= ids, value, 0.0)
                upper[start:start + strip, LANES * t:LANES * t + LANES] = value
            else:
                inverse[start:start + strip, LANES * (t - tiles):LANES * (t - tiles) + LANES] = value
    return emit


def panel_kernel(
    strip, inv_rows, mine_ref, other_ref, panel_hbm, upper_ref, next_ref, parts_hbm,
    panel_ref, parts_ref, inverse_ref, work, moved,
):
    load = pltpu.make_async_copy(panel_hbm, panel_ref, moved.at[0])
    load.start()
    store = pltpu.make_async_copy(parts_ref, parts_hbm, moved.at[1])
    order = upper_ref.shape[0]
    first = lax.axis_index("core") == 0
    row_ids = lax.broadcasted_iota(jnp.int32, (order, order), 0)
    col_ids = lax.broadcasted_iota(jnp.int32, (order, order), 1)

    def block(index):
        area = slice(order * index, order * index + order)
        return jnp.concatenate(ordered(first, mine_ref[:, area], other_ref[:, area]), axis=0) * inv_rows

    work[:, :order] = block(0)
    work[:, order:] = jnp.where(row_ids == col_ids, 1.0, 0.0)
    upper_ref[...] = jnp.zeros_like(upper_ref)
    inverse_ref[...] = jnp.zeros_like(inverse_ref)
    factor(work, order, strip, True, emit_upper(upper_ref, inverse_ref, strip))
    inverse = thirds(inverse_ref[...])
    for index, part in enumerate(inverse):
        parts_ref[index] = part
    load.wait()
    proj = matmul(inverse, thirds(block(1)))
    basis = matmul(thirds(panel_ref[...]), thirds(inverse_ref[...].T))
    for index, part in enumerate(thirds(basis)):
        parts_ref[3 + index] = part
    next_ref[...] = block(2) - matmul(thirds(proj.T), thirds(proj))
    store.start()
    store.wait()


def next_kernel(strip, gram_ref, upper_ref, work):
    order = upper_ref.shape[0]
    work[...] = gram_ref[...]
    upper_ref[...] = jnp.zeros_like(upper_ref)
    factor(work, order, strip, False, emit_upper(upper_ref, None, strip))


def factor_panel(mine, other, panel, inv_rows, strip=16):
    rows, order = panel.shape
    shape = jax.ShapeDtypeStruct((order, order), jnp.float32)
    return pl.pallas_call(
        functools.partial(panel_kernel, strip, inv_rows),
        out_shape=(shape, shape, pltpu.HBM((6, order, order), jnp.bfloat16)),
        in_specs=[VMEM, VMEM, HBM],
        out_specs=(VMEM, VMEM, HBM),
        scratch_shapes=[
            pltpu.VMEM((rows, order), jnp.float32),
            pltpu.VMEM((6, order, order), jnp.bfloat16),
            pltpu.VMEM((order, order), jnp.float32),
            pltpu.VMEM((order, 2 * order), jnp.float32),
            pltpu.SemaphoreType.DMA((2,)),
        ],
        compiler_params=pltpu.CompilerParams(vmem_limit_bytes=VMEM_BYTES),
        cost_estimate=pl.CostEstimate(flops=9 * 10**9, bytes_accessed=6 * 4 * order**2, transcendentals=0),
    )(in_vmem(mine), in_vmem(other), in_hbm(panel))


def factor_next(gram, strip=16):
    order = gram.shape[0]
    return pl.pallas_call(
        functools.partial(next_kernel, strip),
        out_shape=jax.ShapeDtypeStruct((order, order), jnp.float32),
        in_specs=[VMEM],
        out_specs=VMEM,
        scratch_shapes=[pltpu.VMEM((order, order), jnp.float32)],
        compiler_params=pltpu.CompilerParams(vmem_limit_bytes=VMEM_BYTES),
        cost_estimate=pl.CostEstimate(flops=8 * 10**9, bytes_accessed=2 * 4 * order**2, transcendentals=0),
    )(gram)


def split_kernel(stage, mine_a, mine_b, arrived_a, arrived_b, *chunk_refs):
    index = plane_index(stage)
    rows = chunk_refs[0].shape[0]
    cut = mine_a.shape[1]
    for step, chunk_ref in enumerate(chunk_refs):
        area = pl.ds(lax.rem(index + step, 4) * rows, rows)
        chunk_ref[:, :cut] = mine_a[area, :] + arrived_a[area, :]
        chunk_ref[:, cut:] = mine_b[area, :] + arrived_b[area, :]


def add_split(mine, arrived, stage):
    rows = mine[0].shape[0]
    width = mine[0].shape[1] + mine[1].shape[1]
    return pl.pallas_call(
        functools.partial(split_kernel, stage),
        out_shape=(jax.ShapeDtypeStruct((rows // 4, width), jnp.float32),) * 4,
        in_specs=[VMEM] * 4,
        out_specs=(VMEM,) * 4,
        compiler_params=pltpu.CompilerParams(vmem_limit_bytes=VMEM_BYTES),
        cost_estimate=pl.CostEstimate(flops=10**8, bytes_accessed=12 * rows * width, transcendentals=0),
    )(*(in_vmem(value) for value in (*mine, *arrived)))


def update_kernel(
    inv_rows, parts_ref, head_mine, head_other, rest_mine, rest_other, trailing_ref,
    proj_hbm, updated_hbm, proj_ref, updated_ref, sent,
):
    first = lax.axis_index("core") == 0
    width = parts_ref.shape[1]
    count = trailing_ref.shape[1] // width
    areas = [slice(width * t, width * t + width) for t in range(count)]
    inverse = [parts_ref[i] for i in range(3)]
    stores = []

    def project(tile):
        if tile == 0:
            halves = ordered(first, head_mine[:, areas[1]], head_other[:, areas[1]])
        else:
            halves = ordered(first, rest_mine[:, areas[tile - 1]], rest_other[:, areas[tile - 1]])
        proj = matmul(inverse, thirds(jnp.concatenate(halves, axis=0) * inv_rows))
        proj_ref[:, areas[tile]] = proj
        return thirds(proj)

    def send(source, target, tile, slot):
        copy = pltpu.make_async_copy(source.at[:, areas[tile]], target.at[:, areas[tile]], sent.at[slot])
        copy.start()
        stores.append(copy)

    ahead = project(0)
    basis = [parts_ref[i + 3] for i in range(3)]
    for tile in range(count):
        proj = ahead
        if tile + 1 < count:
            ahead = project(tile + 1)
        updated_ref[:, areas[tile]] = trailing_ref[:, areas[tile]] - matmul(basis, proj)
        send(proj_ref, proj_hbm, tile, 2 * tile)
        send(updated_ref, updated_hbm, tile, 2 * tile + 1)
    for copy in stores:
        copy.wait()


def update(parts, grams, rest, trailing, inv_rows):
    width = parts.shape[1]
    rows, columns = trailing.shape
    shapes = ((width, columns), (rows, columns))
    return pl.pallas_call(
        functools.partial(update_kernel, inv_rows),
        out_shape=tuple(jax.ShapeDtypeStruct(shape, jnp.float32) for shape in shapes),
        in_specs=[VMEM] * 6,
        out_specs=(HBM, HBM),
        scratch_shapes=[
            *(pltpu.VMEM(shape, jnp.float32) for shape in shapes),
            pltpu.SemaphoreType.DMA((2 * columns // width,)),
        ],
        compiler_params=pltpu.CompilerParams(vmem_limit_bytes=VMEM_BYTES),
        cost_estimate=pl.CostEstimate(flops=24 * rows * width * columns, bytes_accessed=16 * rows * columns, transcendentals=0),
    )(parts, *grams, *rest, trailing)


ROWS = ("y", "z", "core", "x")


def swap_cores(value):
    return lax.ppermute(value, "core", ((0, 1), (1, 0)))


def plane_shift(value, stage, step):
    pairs = []
    for y, z, core, x in itertools.product(range(4), range(8), range(2), range(4)):
        if core == stage:
            ny, nx = y, (x + step) % 4
        else:
            ny, nx = (y + step) % 4, x
        pairs.append((((y * 8 + z) * 2 + core) * 4 + x, ((ny * 8 + z) * 2 + core) * 4 + nx))
    return lax.ppermute(value, ROWS, pairs)


def plane_index(stage):
    return jnp.where(lax.axis_index("core") == stage, lax.axis_index("x"), lax.axis_index("y"))


def plane_sum(chunks, stage):
    total = chunks[0]
    for step in range(1, 4):
        total = total + plane_shift(chunks[step], stage, step)
    return total


def plane_chunks(value, stage):
    chunks = value.reshape(4, value.shape[0] // 4, value.shape[1])
    index = plane_index(stage)
    return [
        lax.dynamic_index_in_dim(chunks, (index + step) % 4, 0, keepdims=False) for step in range(4)
    ]


def plane_send(value, stage):
    return [value] + [plane_shift(value, stage, step) for step in range(1, 4)]


def plane_join(pieces, stage):
    rows, width = pieces[0].shape
    index = plane_index(stage)
    result = jnp.zeros((4 * rows, width), pieces[0].dtype)
    for step, piece in enumerate(pieces):
        result = lax.dynamic_update_slice(result, piece, ((index + 4 - step) % 4 * rows, 0))
    return result


def plane_spread(piece):
    rows, width = piece.shape
    copies = jnp.broadcast_to(piece[None], (16, rows, width))
    arrived = lax.all_to_all(copies, ("y", "x"), 0, 0, tiled=True).reshape(4, 4, rows, width)
    by_x = jnp.swapaxes(arrived, 0, 1)
    return jnp.where(lax.axis_index("core") == 0, by_x, arrived).reshape(16 * rows, width)


def ring_sum(value):
    for bit in (1, 2, 4):
        value = value + lax.ppermute(value, "z", [(z, z ^ bit) for z in range(8)])
    return value


def per_device(panel, trailing):
    inv_rows = 1.0 / (panel.shape[0] * lax.axis_size(ROWS))
    width = panel.shape[1]
    count = trailing.shape[1] // width
    cut = count // 2 - 1
    mine_a, other_a = products(panel, trailing, 0, cut)
    arrived_a = swap_cores(other_a)
    mine_b, other_b = products(panel, trailing, cut, count)
    arrived_b = swap_cores(other_b)
    piece = plane_sum(add_split((mine_a, mine_b), (arrived_a, arrived_b), 0), 0)
    piece = ring_sum(plane_sum(plane_chunks(piece, 1), 1))
    grams = plane_spread(piece[:, :3 * width])
    grams_other = swap_cores(grams)
    rest_piece = plane_join(plane_send(piece[:, 3 * width:], 1), 1)
    rest_pieces = plane_send(rest_piece, 0)
    upper_panel, gram_next, parts = factor_panel(grams, grams_other, panel, inv_rows)
    rest_pieces, gram_next = lax.optimization_barrier((rest_pieces, gram_next))
    rest = plane_join(rest_pieces, 0)
    rest, gram_next = lax.optimization_barrier((rest, gram_next))
    rest_other = swap_cores(rest)
    upper_next = factor_next(gram_next)
    projection, updated = update(parts, (grams, grams_other), (rest, rest_other), trailing, inv_rows)
    return (upper_panel, projection, updated, upper_next)


def solution(mesh):
    chips = Mesh(mesh.devices.reshape(4, 8, 2, 4), ROWS)
    return jax.shard_map(
        per_device,
        mesh=chips,
        in_specs=(P(ROWS, None), P(ROWS, None)),
        out_specs=(P(), P(), P(ROWS, None), P()),
        check_vma=False,
    )
```

```python
import functools
import itertools
import jax, jax.numpy as jnp
from jax import lax
from jax.experimental import pallas as pl
from jax.experimental.pallas import tpu as pltpu
from jax.sharding import Mesh, PartitionSpec as P

ROWS = "device"
LANES = 128
VMEM_BYTES = 16 * 2**20
VMEM = pl.BlockSpec(memory_space=pltpu.VMEM)
HBM = pl.BlockSpec(memory_space=pltpu.HBM)


in_hbm = functools.partial(pltpu.with_memory_space_constraint, memory_space=pltpu.HBM)
in_vmem = functools.partial(pltpu.with_memory_space_constraint, memory_space=pltpu.VMEM)


def core_index():
    return lax.rem(lax.axis_index(ROWS) // 4, 2)


def row_of(block, row):
    return jnp.broadcast_to(block[row:row + 1, :], block.shape)


def lane_of(block, lane):
    return jnp.broadcast_to(block[:, lane:lane + 1], block.shape)


def thirds(value):
    high = value.astype(jnp.bfloat16)
    rest = value - high.astype(jnp.float32)
    middle = rest.astype(jnp.bfloat16)
    low = (rest - middle.astype(jnp.float32)).astype(jnp.bfloat16)
    return high, middle, low


def matmul(left, right):
    l1, l2, l3 = left
    r1, r2, r3 = right
    pairs = ((l1, r3), (l3, r1), (l2, r2), (l1, r2), (l2, r1), (l1, r1))
    return sum(jnp.dot(a, b, preferred_element_type=jnp.float32) for a, b in pairs)


def outer(left, right):
    l1, l2, l3 = thirds(left)
    r1, r2, r3 = thirds(right)
    return lax.dot_general(
        jnp.concatenate([l1, l1, l2, l2, l1, l3], axis=0),
        jnp.concatenate([r1, r2, r1, r2, r3, r1], axis=0),
        (((0,), (0,)), ((), ())),
        preferred_element_type=jnp.float32,
    )


def factor(work, order, strip, extra, emit):
    groups = strip // 8
    base_tiles = order // LANES
    sub_ids = lax.broadcasted_iota(jnp.int32, (8, LANES), 0)

    def tiles_of(start):
        tiles = list(range(start // LANES, base_tiles))
        if extra:
            tiles += [base_tiles + t for t in range((start + strip + LANES - 1) // LANES)]
        return tiles

    def load(start, group, tile):
        row = start + 8 * group
        return work[row:row + 8, LANES * tile:LANES * tile + LANES]

    rows = {(g, t): load(0, g, t) for g in range(groups) for t in tiles_of(0)}
    for start in range(0, order, strip):
        stop = start + strip
        first, offset = divmod(start, LANES)
        tiles = tiles_of(start)
        active = groups
        if stop < order:
            active = 2 * groups
            for g in range(groups):
                for t in {first, *tiles_of(stop)}:
                    rows[groups + g, t] = load(stop, g, t)
        cols = {
            (m, g): lane_of(rows[g, first], offset + m)
            for m in range(strip) for g in range(m // 8, active)
        }
        scale = [None] * groups
        for j in range(strip):
            g0, s0 = divmod(j, 8)
            inv_root = lax.rsqrt(row_of(cols[j, g0], s0))
            inv = inv_root * inv_root
            scale[g0] = inv_root if s0 == 0 else jnp.where(sub_ids == s0, inv_root, scale[g0])
            mult = {g: cols[j, g] * inv for g in range(g0, active)}
            for m in range(j + 1, strip):
                entry = row_of(cols[j, m // 8], m % 8)
                for g in range(m // 8, active):
                    cols[m, g] = cols[m, g] - mult[g] * entry
            if s0 == 7:
                del mult[g0]
            else:
                mult[g0] = jnp.where(sub_ids > s0, mult[g0], 0.0)
            for t in tiles:
                pivot_row = row_of(rows[g0, t], s0)
                for g in mult:
                    if (g, t) in rows:
                        rows[g, t] = rows[g, t] - mult[g] * pivot_row
        block = {
            t: jnp.concatenate([rows[g, t] * scale[g] for g in range(groups)], axis=0) for t in tiles
        }
        emit(start, block)
        rows = {(g - groups, t): value for (g, t), value in rows.items() if g >= groups}
        after = stop + strip
        if after >= order:
            continue
        base = after // LANES
        left = jnp.concatenate([block[t] for t in range(base, base_tiles)], axis=1)
        keep = [t for t in tiles if t >= stop // LANES]
        change = outer(left, jnp.concatenate([block[t] for t in keep], axis=1))
        for i, t in enumerate(keep):
            area = (slice(after, order), slice(LANES * t, LANES * t + LANES))
            work[area] = work[area] - change[after - LANES * base:, LANES * i:LANES * i + LANES]


def ordered(first, mine, other):
    return jnp.where(first, mine, other), jnp.where(first, other, mine)


def products_kernel(panel_hbm, trailing_hbm, mine_ref, other_ref, panel_ref, trailing_ref, arrived):
    first = core_index() == 0
    width = panel_ref.shape[1]
    half = width // 2
    count = trailing_ref.shape[1] // width
    areas = [slice(width * t, width * t + width) for t in range(count + 2)]
    loads = [pltpu.make_async_copy(panel_hbm, panel_ref, arrived.at[0])]
    for t in range(count):
        loads.append(pltpu.make_async_copy(
            trailing_hbm.at[:, areas[t]], trailing_ref.at[:, areas[t]], arrived.at[t + 1]
        ))
    for load in loads:
        load.start()
    loads[0].wait()
    panel = panel_ref[...]
    left_panel = thirds(panel.T)
    for tile in range(count + 2):
        left = left_panel
        if tile == 0:
            source = panel
        elif tile <= count:
            if tile == 1:
                for load in loads[1:]:
                    load.wait()
            source = trailing_ref[:, areas[tile - 1]]
        else:
            source = trailing_ref[:, areas[0]]
            left = thirds(source.T)
        result = matmul(left, thirds(source))
        mine_ref[:, areas[tile]], other_ref[:, areas[tile]] = ordered(first, result[:half], result[half:])


def products(panel, trailing):
    rows, width = panel.shape
    total = trailing.shape[1] + 2 * width
    shape = jax.ShapeDtypeStruct((width // 2, total), jnp.float32)
    return pl.pallas_call(
        products_kernel,
        out_shape=(shape, shape),
        in_specs=[HBM] * 2,
        out_specs=(VMEM,) * 2,
        scratch_shapes=[
            pltpu.VMEM(panel.shape, jnp.float32),
            pltpu.VMEM(trailing.shape, jnp.float32),
            pltpu.SemaphoreType.DMA((trailing.shape[1] // width + 1,)),
        ],
        compiler_params=pltpu.CompilerParams(vmem_limit_bytes=VMEM_BYTES),
        cost_estimate=pl.CostEstimate(flops=12 * rows * width * total, bytes_accessed=8 * rows * total, transcendentals=0),
    )(in_hbm(panel), in_hbm(trailing))


def emit_upper(upper, inverse, strip):
    tiles = upper.shape[0] // LANES

    def emit(start, block):
        ids = lax.broadcasted_iota(jnp.int32, (strip, LANES), 0) + start
        lanes = lax.broadcasted_iota(jnp.int32, (strip, LANES), 1)
        for t, value in block.items():
            if t < tiles:
                value = jnp.where(lanes + LANES * t >= ids, value, 0.0)
                upper[start:start + strip, LANES * t:LANES * t + LANES] = value
            else:
                inverse[start:start + strip, LANES * (t - tiles):LANES * (t - tiles) + LANES] = value
    return emit


def panel_kernel(
    strip, inv_rows, mine_ref, other_ref, panel_hbm, upper_ref, next_ref, parts_hbm,
    panel_ref, parts_ref, inverse_ref, work, moved,
):
    load = pltpu.make_async_copy(panel_hbm, panel_ref, moved.at[0])
    load.start()
    store = pltpu.make_async_copy(parts_ref, parts_hbm, moved.at[1])
    order = upper_ref.shape[0]
    first = core_index() == 0
    row_ids = lax.broadcasted_iota(jnp.int32, (order, order), 0)
    col_ids = lax.broadcasted_iota(jnp.int32, (order, order), 1)

    def block(index):
        area = slice(order * index, order * index + order)
        return jnp.concatenate(ordered(first, mine_ref[:, area], other_ref[:, area]), axis=0) * inv_rows

    work[:, :order] = block(0)
    work[:, order:] = jnp.where(row_ids == col_ids, 1.0, 0.0)
    upper_ref[...] = jnp.zeros_like(upper_ref)
    inverse_ref[...] = jnp.zeros_like(inverse_ref)
    factor(work, order, strip, True, emit_upper(upper_ref, inverse_ref, strip))
    inverse = thirds(inverse_ref[...])
    for index, part in enumerate(inverse):
        parts_ref[index] = part
    load.wait()
    proj = matmul(inverse, thirds(block(1)))
    basis = matmul(thirds(panel_ref[...]), thirds(inverse_ref[...].T))
    for index, part in enumerate(thirds(basis)):
        parts_ref[3 + index] = part
    next_ref[...] = block(2) - matmul(thirds(proj.T), thirds(proj))
    store.start()
    store.wait()


def next_kernel(strip, gram_ref, upper_ref, work):
    order = upper_ref.shape[0]
    work[...] = gram_ref[...]
    upper_ref[...] = jnp.zeros_like(upper_ref)
    factor(work, order, strip, False, emit_upper(upper_ref, None, strip))


def factor_panel(mine, other, panel, inv_rows, strip=16):
    rows, order = panel.shape
    shape = jax.ShapeDtypeStruct((order, order), jnp.float32)
    return pl.pallas_call(
        functools.partial(panel_kernel, strip, inv_rows),
        out_shape=(shape, shape, pltpu.HBM((6, order, order), jnp.bfloat16)),
        in_specs=[VMEM, VMEM, HBM],
        out_specs=(VMEM, VMEM, HBM),
        scratch_shapes=[
            pltpu.VMEM((rows, order), jnp.float32),
            pltpu.VMEM((6, order, order), jnp.bfloat16),
            pltpu.VMEM((order, order), jnp.float32),
            pltpu.VMEM((order, 2 * order), jnp.float32),
            pltpu.SemaphoreType.DMA((2,)),
        ],
        compiler_params=pltpu.CompilerParams(vmem_limit_bytes=VMEM_BYTES),
        cost_estimate=pl.CostEstimate(flops=9 * 10**9, bytes_accessed=6 * 4 * order**2, transcendentals=0),
    )(in_vmem(mine), in_vmem(other), in_hbm(panel))


def factor_next(gram, strip=16):
    order = gram.shape[0]
    return pl.pallas_call(
        functools.partial(next_kernel, strip),
        out_shape=jax.ShapeDtypeStruct((order, order), jnp.float32),
        in_specs=[VMEM],
        out_specs=VMEM,
        scratch_shapes=[pltpu.VMEM((order, order), jnp.float32)],
        compiler_params=pltpu.CompilerParams(vmem_limit_bytes=VMEM_BYTES),
        cost_estimate=pl.CostEstimate(flops=8 * 10**9, bytes_accessed=2 * 4 * order**2, transcendentals=0),
    )(gram)


def add_kernel(mine_ref, arrived_ref, total_ref):
    total_ref[...] = mine_ref[...] + arrived_ref[...]


def add_halves(mine, arrived):
    return pl.pallas_call(
        add_kernel,
        out_shape=jax.ShapeDtypeStruct(mine.shape, jnp.float32),
        in_specs=[VMEM] * 2,
        out_specs=VMEM,
        compiler_params=pltpu.CompilerParams(vmem_limit_bytes=VMEM_BYTES),
        cost_estimate=pl.CostEstimate(flops=10**8, bytes_accessed=12 * mine.size, transcendentals=0),
    )(in_vmem(mine), in_vmem(arrived))


def update_kernel(
    inv_rows, parts_ref, head_mine, head_other, rest_mine, rest_other, trailing_ref,
    proj_hbm, updated_hbm, proj_ref, updated_ref, sent,
):
    first = core_index() == 0
    width = parts_ref.shape[1]
    count = trailing_ref.shape[1] // width
    areas = [slice(width * t, width * t + width) for t in range(count)]
    inverse = [parts_ref[i] for i in range(3)]
    stores = []

    def project(tile):
        if tile == 0:
            halves = ordered(first, head_mine[:, areas[1]], head_other[:, areas[1]])
        else:
            halves = ordered(first, rest_mine[:, areas[tile - 1]], rest_other[:, areas[tile - 1]])
        proj = matmul(inverse, thirds(jnp.concatenate(halves, axis=0) * inv_rows))
        proj_ref[:, areas[tile]] = proj
        return thirds(proj)

    def send(source, target, tile, slot):
        copy = pltpu.make_async_copy(source.at[:, areas[tile]], target.at[:, areas[tile]], sent.at[slot])
        copy.start()
        stores.append(copy)

    ahead = project(0)
    basis = [parts_ref[i + 3] for i in range(3)]
    for tile in range(count):
        proj = ahead
        if tile + 1 < count:
            ahead = project(tile + 1)
        updated_ref[:, areas[tile]] = trailing_ref[:, areas[tile]] - matmul(basis, proj)
        send(proj_ref, proj_hbm, tile, 2 * tile)
        send(updated_ref, updated_hbm, tile, 2 * tile + 1)
    for copy in stores:
        copy.wait()


def update(parts, grams, rest, trailing, inv_rows):
    width = parts.shape[1]
    rows, columns = trailing.shape
    shapes = ((width, columns), (rows, columns))
    return pl.pallas_call(
        functools.partial(update_kernel, inv_rows),
        out_shape=tuple(jax.ShapeDtypeStruct(shape, jnp.float32) for shape in shapes),
        in_specs=[VMEM] * 6,
        out_specs=(HBM, HBM),
        scratch_shapes=[
            *(pltpu.VMEM(shape, jnp.float32) for shape in shapes),
            pltpu.SemaphoreType.DMA((2 * columns // width,)),
        ],
        compiler_params=pltpu.CompilerParams(vmem_limit_bytes=VMEM_BYTES),
        cost_estimate=pl.CostEstimate(flops=24 * rows * width * columns, bytes_accessed=16 * rows * columns, transcendentals=0),
    )(parts, *grams, *rest, trailing)


def swap_cores(value):
    return lax.ppermute(value, ROWS, [(d, d ^ 4) for d in range(256)])


def plane_groups(stage):
    groups = []
    for z, core, other in itertools.product(range(8), range(2), range(4)):
        members = []
        for k in range(4):
            y, x = (other, k) if core == stage else (k, other)
            members.append(((y * 8 + z) * 2 + core) * 4 + x)
        groups.append(members)
    return groups


def plane_exchange(value, stage):
    return lax.all_to_all(value, ROWS, 0, 0, axis_index_groups=plane_groups(stage), tiled=True)


def plane_sum(value, stage):
    chunks = value.reshape(4, value.shape[0] // 4, value.shape[1])
    return jnp.sum(plane_exchange(chunks, stage), axis=0)


def plane_gather(value, stage):
    copies = jnp.broadcast_to(value[None], (4,) + value.shape)
    return plane_exchange(copies, stage)


def ring_sum(value):
    for bit in (1, 2, 4):
        value = value + lax.ppermute(value, ROWS, [(d, d ^ (8 * bit)) for d in range(256)])
    return value


def per_device(panel, trailing):
    inv_rows = 1.0 / (panel.shape[0] * lax.axis_size(ROWS))
    width = panel.shape[1]
    columns = trailing.shape[1]
    mine, other = products(panel, trailing)
    piece = plane_sum(add_halves(mine, swap_cores(other)), 0)
    piece = ring_sum(plane_sum(piece, 1))
    piece = plane_gather(piece, 1).reshape(32, -1)
    first_part = jnp.concatenate([piece[:, :2 * width], piece[:, columns + width:]], axis=1)
    grams = plane_gather(first_part, 0).reshape(128, -1)
    grams_other = swap_cores(grams)
    rest = plane_gather(piece[:, 2 * width:columns + width], 0)
    upper_panel, gram_next, parts = factor_panel(grams, grams_other, panel, inv_rows)
    rest, gram_next = lax.optimization_barrier((rest, gram_next))
    rest = rest.reshape(128, -1)
    rest_other = swap_cores(rest)
    upper_next = factor_next(gram_next)
    projection, updated = update(parts, (grams, grams_other), (rest, rest_other), trailing, inv_rows)
    return (upper_panel, projection, updated, upper_next)


def solution(mesh):
    chips = Mesh(mesh.devices.reshape(256), (ROWS,))
    return jax.shard_map(
        per_device,
        mesh=chips,
        in_specs=(P(ROWS, None), P(ROWS, None)),
        out_specs=(P(), P(), P(ROWS, None), P()),
        check_vma=False,
    )
```

```python
import functools
import itertools
import jax, jax.numpy as jnp
from jax import lax
from jax.experimental import pallas as pl
from jax.experimental.pallas import tpu as pltpu
from jax.sharding import Mesh, PartitionSpec as P


PLANE_STEPS = (2, 1, 3)
LANES = 128
VMEM_BYTES = 16 * 2**20
VMEM = pl.BlockSpec(memory_space=pltpu.VMEM)
HBM = pl.BlockSpec(memory_space=pltpu.HBM)


in_hbm = functools.partial(pltpu.with_memory_space_constraint, memory_space=pltpu.HBM)
in_vmem = functools.partial(pltpu.with_memory_space_constraint, memory_space=pltpu.VMEM)


def row_of(block, row):
    return jnp.broadcast_to(block[row:row + 1, :], block.shape)


def lane_of(block, lane):
    return jnp.broadcast_to(block[:, lane:lane + 1], block.shape)


def thirds(value):
    high = value.astype(jnp.bfloat16)
    rest = value - high.astype(jnp.float32)
    middle = rest.astype(jnp.bfloat16)
    low = (rest - middle.astype(jnp.float32)).astype(jnp.bfloat16)
    return high, middle, low


def matmul(left, right):
    l1, l2, l3 = left
    r1, r2, r3 = right
    pairs = ((l1, r3), (l3, r1), (l2, r2), (l1, r2), (l2, r1), (l1, r1))
    return sum(jnp.dot(a, b, preferred_element_type=jnp.float32) for a, b in pairs)


def outer(left, right):
    l1, l2, l3 = thirds(left)
    r1, r2, r3 = thirds(right)
    return lax.dot_general(
        jnp.concatenate([l1, l1, l2, l2, l1, l3], axis=0),
        jnp.concatenate([r1, r2, r1, r2, r3, r1], axis=0),
        (((0,), (0,)), ((), ())),
        preferred_element_type=jnp.float32,
    )


def factor(work, order, strip, extra, emit):
    groups = strip // 8
    base_tiles = order // LANES
    sub_ids = lax.broadcasted_iota(jnp.int32, (8, LANES), 0)

    def tiles_of(start):
        tiles = list(range(start // LANES, base_tiles))
        if extra:
            tiles += [base_tiles + t for t in range((start + strip + LANES - 1) // LANES)]
        return tiles

    def load(start, group, tile):
        row = start + 8 * group
        return work[row:row + 8, LANES * tile:LANES * tile + LANES]

    rows = {(g, t): load(0, g, t) for g in range(groups) for t in tiles_of(0)}
    for start in range(0, order, strip):
        stop = start + strip
        first, offset = divmod(start, LANES)
        tiles = tiles_of(start)
        active = groups
        if stop < order:
            active = 2 * groups
            for g in range(groups):
                for t in {first, *tiles_of(stop)}:
                    rows[groups + g, t] = load(stop, g, t)
        cols = {
            (m, g): lane_of(rows[g, first], offset + m)
            for m in range(strip) for g in range(m // 8, active)
        }
        scale = [None] * groups
        for j in range(strip):
            g0, s0 = divmod(j, 8)
            inv_root = lax.rsqrt(row_of(cols[j, g0], s0))
            inv = inv_root * inv_root
            scale[g0] = inv_root if s0 == 0 else jnp.where(sub_ids == s0, inv_root, scale[g0])
            mult = {g: cols[j, g] * inv for g in range(g0, active)}
            for m in range(j + 1, strip):
                entry = row_of(cols[j, m // 8], m % 8)
                for g in range(m // 8, active):
                    cols[m, g] = cols[m, g] - mult[g] * entry
            if s0 == 7:
                del mult[g0]
            else:
                mult[g0] = jnp.where(sub_ids > s0, mult[g0], 0.0)
            for t in tiles:
                pivot_row = row_of(rows[g0, t], s0)
                for g in mult:
                    if (g, t) in rows:
                        rows[g, t] = rows[g, t] - mult[g] * pivot_row
        block = {
            t: jnp.concatenate([rows[g, t] * scale[g] for g in range(groups)], axis=0) for t in tiles
        }
        emit(start, block)
        rows = {(g - groups, t): value for (g, t), value in rows.items() if g >= groups}
        after = stop + strip
        if after >= order:
            continue
        base = after // LANES
        left = jnp.concatenate([block[t] for t in range(base, base_tiles)], axis=1)
        keep = [t for t in tiles if t >= stop // LANES]
        change = outer(left, jnp.concatenate([block[t] for t in keep], axis=1))
        for i, t in enumerate(keep):
            area = (slice(after, order), slice(LANES * t, LANES * t + LANES))
            work[area] = work[area] - change[after - LANES * base:, LANES * i:LANES * i + LANES]


def ordered(first, mine, other):
    return jnp.where(first, mine, other), jnp.where(first, other, mine)


def products_kernel(panel_hbm, trailing_hbm, mine_ref, other_ref, panel_ref, trailing_ref, arrived):
    first = lax.axis_index("core") == 0
    width = panel_ref.shape[1]
    half = width // 2
    count = trailing_ref.shape[1] // width
    areas = [slice(width * t, width * t + width) for t in range(count + 2)]
    loads = [pltpu.make_async_copy(panel_hbm, panel_ref, arrived.at[0])]
    for t in range(count):
        loads.append(pltpu.make_async_copy(
            trailing_hbm.at[:, areas[t]], trailing_ref.at[:, areas[t]], arrived.at[t + 1]
        ))
    for load in loads:
        load.start()
    loads[0].wait()
    panel = panel_ref[...]
    left_panel = thirds(panel.T)
    for tile in range(count + 2):
        left = left_panel
        if tile == 0:
            source = panel
        elif tile <= count:
            if tile == 1:
                for load in loads[1:]:
                    load.wait()
            source = trailing_ref[:, areas[tile - 1]]
        else:
            source = trailing_ref[:, areas[0]]
            left = thirds(source.T)
        result = matmul(left, thirds(source))
        mine_ref[:, areas[tile]], other_ref[:, areas[tile]] = ordered(first, result[:half], result[half:])


def products(panel, trailing):
    rows, width = panel.shape
    total = trailing.shape[1] + 2 * width
    shape = jax.ShapeDtypeStruct((width // 2, total), jnp.float32)
    return pl.pallas_call(
        products_kernel,
        out_shape=(shape, shape),
        in_specs=[HBM] * 2,
        out_specs=(VMEM,) * 2,
        scratch_shapes=[
            pltpu.VMEM(panel.shape, jnp.float32),
            pltpu.VMEM(trailing.shape, jnp.float32),
            pltpu.SemaphoreType.DMA((trailing.shape[1] // width + 1,)),
        ],
        compiler_params=pltpu.CompilerParams(vmem_limit_bytes=VMEM_BYTES),
        cost_estimate=pl.CostEstimate(flops=12 * rows * width * total, bytes_accessed=8 * rows * total, transcendentals=0),
    )(in_hbm(panel), in_hbm(trailing))


def emit_upper(upper, inverse, strip):
    tiles = upper.shape[0] // LANES

    def emit(start, block):
        ids = lax.broadcasted_iota(jnp.int32, (strip, LANES), 0) + start
        lanes = lax.broadcasted_iota(jnp.int32, (strip, LANES), 1)
        for t, value in block.items():
            if t < tiles:
                value = jnp.where(lanes + LANES * t >= ids, value, 0.0)
                upper[start:start + strip, LANES * t:LANES * t + LANES] = value
            else:
                inverse[start:start + strip, LANES * (t - tiles):LANES * (t - tiles) + LANES] = value

    return emit


def panel_kernel(
    strip, inv_rows, mine_ref, other_ref, panel_hbm, upper_ref, next_ref, parts_hbm,
    panel_ref, parts_ref, inverse_ref, work, moved,
):
    load = pltpu.make_async_copy(panel_hbm, panel_ref, moved.at[0])
    load.start()
    store = pltpu.make_async_copy(parts_ref, parts_hbm, moved.at[1])
    order = upper_ref.shape[0]
    first = lax.axis_index("core") == 0
    row_ids = lax.broadcasted_iota(jnp.int32, (order, order), 0)
    col_ids = lax.broadcasted_iota(jnp.int32, (order, order), 1)

    def block(index):
        area = slice(order * index, order * index + order)
        return jnp.concatenate(ordered(first, mine_ref[:, area], other_ref[:, area]), axis=0) * inv_rows

    work[:, :order] = block(0)
    work[:, order:] = jnp.where(row_ids == col_ids, 1.0, 0.0)
    upper_ref[...] = jnp.zeros_like(upper_ref)
    inverse_ref[...] = jnp.zeros_like(inverse_ref)
    factor(work, order, strip, True, emit_upper(upper_ref, inverse_ref, strip))
    inverse = thirds(inverse_ref[...])
    for index, part in enumerate(inverse):
        parts_ref[index] = part
    load.wait()
    proj = matmul(inverse, thirds(block(1)))
    basis = matmul(thirds(panel_ref[...]), thirds(inverse_ref[...].T))
    for index, part in enumerate(thirds(basis)):
        parts_ref[3 + index] = part
    next_ref[...] = block(2) - matmul(thirds(proj.T), thirds(proj))
    store.start()
    store.wait()


def next_kernel(strip, gram_ref, upper_ref, work):
    order = upper_ref.shape[0]
    work[...] = gram_ref[...]
    upper_ref[...] = jnp.zeros_like(upper_ref)
    factor(work, order, strip, False, emit_upper(upper_ref, None, strip))


def factor_panel(mine, other, panel, inv_rows, strip=16):
    rows, order = panel.shape
    shape = jax.ShapeDtypeStruct((order, order), jnp.float32)
    return pl.pallas_call(
        functools.partial(panel_kernel, strip, inv_rows),
        out_shape=(shape, shape, pltpu.HBM((6, order, order), jnp.bfloat16)),
        in_specs=[VMEM, VMEM, HBM],
        out_specs=(VMEM, VMEM, HBM),
        scratch_shapes=[
            pltpu.VMEM((rows, order), jnp.float32),
            pltpu.VMEM((6, order, order), jnp.bfloat16),
            pltpu.VMEM((order, order), jnp.float32),
            pltpu.VMEM((order, 2 * order), jnp.float32),
            pltpu.SemaphoreType.DMA((2,)),
        ],
        compiler_params=pltpu.CompilerParams(vmem_limit_bytes=VMEM_BYTES),
        cost_estimate=pl.CostEstimate(flops=9 * 10**9, bytes_accessed=6 * 4 * order**2, transcendentals=0),
    )(in_vmem(mine), in_vmem(other), in_hbm(panel))


def factor_next(gram, strip=16):
    order = gram.shape[0]
    return pl.pallas_call(
        functools.partial(next_kernel, strip),
        out_shape=jax.ShapeDtypeStruct((order, order), jnp.float32),
        in_specs=[VMEM],
        out_specs=VMEM,
        scratch_shapes=[pltpu.VMEM((order, order), jnp.float32)],
        compiler_params=pltpu.CompilerParams(vmem_limit_bytes=VMEM_BYTES),
        cost_estimate=pl.CostEstimate(flops=8 * 10**9, bytes_accessed=2 * 4 * order**2, transcendentals=0),
    )(gram)


def split_kernel(stage, mine_ref, arrived_ref, *chunk_refs):
    index = plane_index(stage)
    rows = chunk_refs[0].shape[0]
    for step, chunk_ref in enumerate(chunk_refs):
        area = pl.ds(lax.rem(index + step, 4) * rows, rows)
        chunk_ref[...] = mine_ref[area, :] + arrived_ref[area, :]


def add_split(mine, arrived, stage):
    rows, width = mine.shape
    return pl.pallas_call(
        functools.partial(split_kernel, stage),
        out_shape=(jax.ShapeDtypeStruct((rows // 4, width), jnp.float32),) * 4,
        in_specs=[VMEM] * 2,
        out_specs=(VMEM,) * 4,
        compiler_params=pltpu.CompilerParams(vmem_limit_bytes=VMEM_BYTES),
        cost_estimate=pl.CostEstimate(flops=10**8, bytes_accessed=12 * rows * width, transcendentals=0),
    )(in_vmem(mine), in_vmem(arrived))


def update_kernel(
    inv_rows, parts_ref, head_mine, head_other, rest_mine, rest_other, trailing_ref,
    proj_hbm, updated_hbm, proj_ref, updated_ref, sent,
):
    first = lax.axis_index("core") == 0
    width = parts_ref.shape[1]
    count = trailing_ref.shape[1] // width
    areas = [slice(width * t, width * t + width) for t in range(count)]
    inverse = [parts_ref[i] for i in range(3)]
    stores = []

    def project(tile):
        if tile == 0:
            halves = ordered(first, head_mine[:, areas[1]], head_other[:, areas[1]])
        else:
            halves = ordered(first, rest_mine[:, areas[tile - 1]], rest_other[:, areas[tile - 1]])
        proj = matmul(inverse, thirds(jnp.concatenate(halves, axis=0) * inv_rows))
        proj_ref[:, areas[tile]] = proj
        return thirds(proj)

    def send(source, target, tile, slot):
        copy = pltpu.make_async_copy(source.at[:, areas[tile]], target.at[:, areas[tile]], sent.at[slot])
        copy.start()
        stores.append(copy)

    ahead = project(0)
    basis = [parts_ref[i + 3] for i in range(3)]
    for tile in range(count):
        proj = ahead
        if tile + 1 < count:
            ahead = project(tile + 1)
        updated_ref[:, areas[tile]] = trailing_ref[:, areas[tile]] - matmul(basis, proj)
        send(proj_ref, proj_hbm, tile, 2 * tile)
        send(updated_ref, updated_hbm, tile, 2 * tile + 1)
    for copy in stores:
        copy.wait()


def update(parts, grams, rest, trailing, inv_rows):
    width = parts.shape[1]
    rows, columns = trailing.shape
    shapes = ((width, columns), (rows, columns))
    return pl.pallas_call(
        functools.partial(update_kernel, inv_rows),
        out_shape=tuple(jax.ShapeDtypeStruct(shape, jnp.float32) for shape in shapes),
        in_specs=[VMEM] * 6,
        out_specs=(HBM, HBM),
        scratch_shapes=[
            *(pltpu.VMEM(shape, jnp.float32) for shape in shapes),
            pltpu.SemaphoreType.DMA((2 * columns // width,)),
        ],
        compiler_params=pltpu.CompilerParams(vmem_limit_bytes=VMEM_BYTES),
        cost_estimate=pl.CostEstimate(flops=24 * rows * width * columns, bytes_accessed=16 * rows * columns, transcendentals=0),
    )(parts, *grams, *rest, trailing)


ROWS = ("y", "z", "core", "x")


def swap_cores(value):
    return lax.ppermute(value, "core", ((0, 1), (1, 0)))


def plane_shift(value, stage, step):
    pairs = []
    for y, z, core, x in itertools.product(range(4), range(8), range(2), range(4)):
        if core == stage:
            ny, nx = y, (x + step) % 4
        else:
            ny, nx = (y + step) % 4, x
        pairs.append((((y * 8 + z) * 2 + core) * 4 + x, ((ny * 8 + z) * 2 + core) * 4 + nx))
    return lax.ppermute(value, ROWS, pairs)


def plane_index(stage):
    return jnp.where(lax.axis_index("core") == stage, lax.axis_index("x"), lax.axis_index("y"))


def plane_sum(chunks, stage):
    total = chunks[0]
    for step in PLANE_STEPS:
        total = total + plane_shift(chunks[step], stage, step)
    return total


def plane_chunks(value, stage):
    chunks = value.reshape(4, value.shape[0] // 4, value.shape[1])
    index = plane_index(stage)
    return [
        lax.dynamic_index_in_dim(chunks, (index + step) % 4, 0, keepdims=False) for step in range(4)
    ]


def plane_send(value, stage):
    return [value] + [plane_shift(value, stage, step) for step in PLANE_STEPS]


def plane_join(pieces, stage):
    rows, width = pieces[0].shape
    index = plane_index(stage)
    result = jnp.zeros((4 * rows, width), pieces[0].dtype)
    for step, piece in zip((0, *PLANE_STEPS), pieces):
        result = lax.dynamic_update_slice(result, piece, ((index + 4 - step) % 4 * rows, 0))
    return result


def ring_sum(value):
    for bit in (1, 2, 4):
        value = value + lax.ppermute(value, "z", [(z, z ^ bit) for z in range(8)])
    return value


def per_device(panel, trailing):
    inv_rows = 1.0 / (panel.shape[0] * lax.axis_size(ROWS))
    width = panel.shape[1]
    columns = trailing.shape[1]
    mine, other = products(panel, trailing)
    piece = plane_sum(add_split(mine, swap_cores(other), 0), 0)
    piece = ring_sum(plane_sum(plane_chunks(piece, 1), 1))
    piece = plane_join(plane_send(piece, 1), 1)
    first_part = jnp.concatenate([piece[:, :2 * width], piece[:, columns + width:]], axis=1)
    gram_pieces = plane_send(first_part, 0)
    rest_pieces = plane_send(piece[:, 2 * width:columns + width], 0)
    grams = plane_join(gram_pieces, 0)
    grams_other = swap_cores(grams)
    upper_panel, gram_next, parts = factor_panel(grams, grams_other, panel, inv_rows)
    rest_pieces, gram_next = lax.optimization_barrier((rest_pieces, gram_next))
    rest = plane_join(rest_pieces, 0)
    rest, gram_next = lax.optimization_barrier((rest, gram_next))
    rest_other = swap_cores(rest)
    upper_next = factor_next(gram_next)
    projection, updated = update(parts, (grams, grams_other), (rest, rest_other), trailing, inv_rows)
    return (upper_panel, projection, updated, upper_next)


def solution(mesh):
    chips = Mesh(mesh.devices.reshape(4, 8, 2, 4), ROWS)

    return jax.shard_map(
        per_device,
        mesh=chips,
        in_specs=(P(ROWS, None), P(ROWS, None)),
        out_specs=(P(), P(), P(ROWS, None), P()),
        check_vma=False,
    )
```

```python
import functools
import itertools
import jax, jax.numpy as jnp
from jax import lax
from jax.experimental import pallas as pl
from jax.experimental.pallas import tpu as pltpu
from jax.sharding import Mesh, PartitionSpec as P


PLANE_STEPS = (2, 1, 3)
LANES = 128
VMEM_BYTES = 16 * 2**20
VMEM = pl.BlockSpec(memory_space=pltpu.VMEM)
HBM = pl.BlockSpec(memory_space=pltpu.HBM)


in_hbm = functools.partial(pltpu.with_memory_space_constraint, memory_space=pltpu.HBM)
in_vmem = functools.partial(pltpu.with_memory_space_constraint, memory_space=pltpu.VMEM)


def row_of(block, row):
    return jnp.broadcast_to(block[row:row + 1, :], block.shape)


def lane_of(block, lane):
    return jnp.broadcast_to(block[:, lane:lane + 1], block.shape)


def thirds(value):
    high = value.astype(jnp.bfloat16)
    rest = value - high.astype(jnp.float32)
    middle = rest.astype(jnp.bfloat16)
    low = (rest - middle.astype(jnp.float32)).astype(jnp.bfloat16)
    return high, middle, low


def matmul(left, right):
    l1, l2, l3 = left
    r1, r2, r3 = right
    pairs = ((l1, r3), (l3, r1), (l2, r2), (l1, r2), (l2, r1), (l1, r1))
    return sum(jnp.dot(a, b, preferred_element_type=jnp.float32) for a, b in pairs)


def outer(left, right):
    l1, l2, l3 = thirds(left)
    r1, r2, r3 = thirds(right)
    return lax.dot_general(
        jnp.concatenate([l1, l1, l2, l2, l1, l3], axis=0),
        jnp.concatenate([r1, r2, r1, r2, r3, r1], axis=0),
        (((0,), (0,)), ((), ())),
        preferred_element_type=jnp.float32,
    )


def factor(work, order, strip, extra, emit):
    groups = strip // 8
    base_tiles = order // LANES
    sub_ids = lax.broadcasted_iota(jnp.int32, (8, LANES), 0)

    def tiles_of(start):
        tiles = list(range(start // LANES, base_tiles))
        if extra:
            tiles += [base_tiles + t for t in range((start + strip + LANES - 1) // LANES)]
        return tiles

    def load(start, group, tile):
        row = start + 8 * group
        return work[row:row + 8, LANES * tile:LANES * tile + LANES]

    rows = {(g, t): load(0, g, t) for g in range(groups) for t in tiles_of(0)}
    for start in range(0, order, strip):
        stop = start + strip
        first, offset = divmod(start, LANES)
        tiles = tiles_of(start)
        active = groups
        if stop < order:
            active = 2 * groups
            for g in range(groups):
                for t in {first, *tiles_of(stop)}:
                    rows[groups + g, t] = load(stop, g, t)
        cols = {
            (m, g): lane_of(rows[g, first], offset + m)
            for m in range(strip) for g in range(m // 8, active)
        }
        scale = [None] * groups
        for j in range(strip):
            g0, s0 = divmod(j, 8)
            inv_root = lax.rsqrt(row_of(cols[j, g0], s0))
            inv = inv_root * inv_root
            scale[g0] = inv_root if s0 == 0 else jnp.where(sub_ids == s0, inv_root, scale[g0])
            mult = {g: cols[j, g] * inv for g in range(g0, active)}
            for m in range(j + 1, strip):
                entry = row_of(cols[j, m // 8], m % 8)
                for g in range(m // 8, active):
                    cols[m, g] = cols[m, g] - mult[g] * entry
            if s0 == 7:
                del mult[g0]
            else:
                mult[g0] = jnp.where(sub_ids > s0, mult[g0], 0.0)
            for t in tiles:
                pivot_row = row_of(rows[g0, t], s0)
                for g in mult:
                    if (g, t) in rows:
                        rows[g, t] = rows[g, t] - mult[g] * pivot_row
        block = {
            t: jnp.concatenate([rows[g, t] * scale[g] for g in range(groups)], axis=0) for t in tiles
        }
        emit(start, block)
        rows = {(g - groups, t): value for (g, t), value in rows.items() if g >= groups}
        after = stop + strip
        if after >= order:
            continue
        base = after // LANES
        left = jnp.concatenate([block[t] for t in range(base, base_tiles)], axis=1)
        keep = [t for t in tiles if t >= stop // LANES]
        change = outer(left, jnp.concatenate([block[t] for t in keep], axis=1))
        for i, t in enumerate(keep):
            area = (slice(after, order), slice(LANES * t, LANES * t + LANES))
            work[area] = work[area] - change[after - LANES * base:, LANES * i:LANES * i + LANES]


def ordered(first, mine, other):
    return jnp.where(first, mine, other), jnp.where(first, other, mine)


def put_product(first, mine_ref, other_ref, slot, left, source):
    width = source.shape[1]
    area = slice(width * slot, width * slot + width)
    result = matmul(left, thirds(source))
    half = width // 2
    mine_ref[:, area], other_ref[:, area] = ordered(first, result[:half], result[half:])


def gram_kernel(
    panel_hbm, trailing_hbm, mine_ref, other_ref, left_ref, late_ref, panel_ref, early_ref, arrived,
):
    first = lax.axis_index("core") == 0
    width = panel_ref.shape[1]
    cut = early_ref.shape[1]
    loads = [
        pltpu.make_async_copy(panel_hbm, panel_ref, arrived.at[0]),
        pltpu.make_async_copy(trailing_hbm.at[:, :cut], early_ref, arrived.at[1]),
        pltpu.make_async_copy(trailing_hbm.at[:, cut:], late_ref, arrived.at[2]),
    ]
    for load in loads:
        load.start()
    loads[0].wait()
    panel = panel_ref[...]
    left = thirds(panel.T)
    for index, part in enumerate(left):
        left_ref[index] = part
    put_product(first, mine_ref, other_ref, 0, left, panel)
    loads[1].wait()
    head = early_ref[:, :width]
    put_product(first, mine_ref, other_ref, 1, left, head)
    put_product(first, mine_ref, other_ref, 2, thirds(head.T), head)
    for tile in range(1, cut // width):
        put_product(first, mine_ref, other_ref, tile + 2, left, early_ref[:, width * tile:width * tile + width])
    loads[2].wait()


def late_kernel(left_ref, late_ref, mine_ref, other_ref):
    first = lax.axis_index("core") == 0
    width = left_ref.shape[2]
    left = [left_ref[index] for index in range(3)]
    for tile in range(late_ref.shape[1] // width):
        put_product(first, mine_ref, other_ref, tile, left, late_ref[:, width * tile:width * tile + width])


def early_products(panel, trailing, cut):
    rows, width = panel.shape
    late = trailing.shape[1] - cut
    shape = jax.ShapeDtypeStruct((width // 2, cut + 2 * width), jnp.float32)
    return pl.pallas_call(
        gram_kernel,
        out_shape=(
            shape, shape, pltpu.VMEM((3, width, rows), jnp.bfloat16), pltpu.VMEM((rows, late), jnp.float32),
        ),
        in_specs=[HBM] * 2,
        out_specs=(VMEM,) * 4,
        scratch_shapes=[
            pltpu.VMEM(panel.shape, jnp.float32),
            pltpu.VMEM((rows, cut), jnp.float32),
            pltpu.SemaphoreType.DMA((3,)),
        ],
        compiler_params=pltpu.CompilerParams(vmem_limit_bytes=VMEM_BYTES),
        cost_estimate=pl.CostEstimate(flops=2 * 10**9, bytes_accessed=8 * rows * trailing.shape[1], transcendentals=0),
    )(in_hbm(panel), in_hbm(trailing))


def late_products(left, late):
    width = left.shape[1]
    shape = jax.ShapeDtypeStruct((width // 2, late.shape[1]), jnp.float32)
    return pl.pallas_call(
        late_kernel,
        out_shape=(shape, shape),
        in_specs=[VMEM] * 2,
        out_specs=(VMEM,) * 2,
        compiler_params=pltpu.CompilerParams(vmem_limit_bytes=VMEM_BYTES),
        cost_estimate=pl.CostEstimate(flops=2 * 10**9, bytes_accessed=8 * late.size, transcendentals=0),
    )(in_vmem(left), in_vmem(late))


def emit_upper(upper, inverse, strip):
    tiles = upper.shape[0] // LANES

    def emit(start, block):
        ids = lax.broadcasted_iota(jnp.int32, (strip, LANES), 0) + start
        lanes = lax.broadcasted_iota(jnp.int32, (strip, LANES), 1)
        for t, value in block.items():
            if t < tiles:
                value = jnp.where(lanes + LANES * t >= ids, value, 0.0)
                upper[start:start + strip, LANES * t:LANES * t + LANES] = value
            else:
                inverse[start:start + strip, LANES * (t - tiles):LANES * (t - tiles) + LANES] = value

    return emit


def panel_kernel(
    strip, inv_rows, mine_ref, other_ref, panel_hbm, upper_ref, next_ref, parts_hbm,
    panel_ref, parts_ref, inverse_ref, work, moved,
):
    load = pltpu.make_async_copy(panel_hbm, panel_ref, moved.at[0])
    load.start()
    store = pltpu.make_async_copy(parts_ref, parts_hbm, moved.at[1])
    order = upper_ref.shape[0]
    first = lax.axis_index("core") == 0
    row_ids = lax.broadcasted_iota(jnp.int32, (order, order), 0)
    col_ids = lax.broadcasted_iota(jnp.int32, (order, order), 1)

    def block(index):
        area = slice(order * index, order * index + order)
        return jnp.concatenate(ordered(first, mine_ref[:, area], other_ref[:, area]), axis=0) * inv_rows

    work[:, :order] = block(0)
    work[:, order:] = jnp.where(row_ids == col_ids, 1.0, 0.0)
    upper_ref[...] = jnp.zeros_like(upper_ref)
    inverse_ref[...] = jnp.zeros_like(inverse_ref)
    factor(work, order, strip, True, emit_upper(upper_ref, inverse_ref, strip))
    inverse = thirds(inverse_ref[...])
    for index, part in enumerate(inverse):
        parts_ref[index] = part
    load.wait()
    proj = matmul(inverse, thirds(block(1)))
    basis = matmul(thirds(panel_ref[...]), thirds(inverse_ref[...].T))
    for index, part in enumerate(thirds(basis)):
        parts_ref[3 + index] = part
    next_ref[...] = block(2) - matmul(thirds(proj.T), thirds(proj))
    store.start()
    store.wait()


def next_kernel(strip, gram_ref, upper_ref, work):
    order = upper_ref.shape[0]
    work[...] = gram_ref[...]
    upper_ref[...] = jnp.zeros_like(upper_ref)
    factor(work, order, strip, False, emit_upper(upper_ref, None, strip))


def factor_panel(mine, other, panel, inv_rows, strip=16):
    rows, order = panel.shape
    shape = jax.ShapeDtypeStruct((order, order), jnp.float32)
    return pl.pallas_call(
        functools.partial(panel_kernel, strip, inv_rows),
        out_shape=(shape, shape, pltpu.HBM((6, order, order), jnp.bfloat16)),
        in_specs=[VMEM, VMEM, HBM],
        out_specs=(VMEM, VMEM, HBM),
        scratch_shapes=[
            pltpu.VMEM((rows, order), jnp.float32),
            pltpu.VMEM((6, order, order), jnp.bfloat16),
            pltpu.VMEM((order, order), jnp.float32),
            pltpu.VMEM((order, 2 * order), jnp.float32),
            pltpu.SemaphoreType.DMA((2,)),
        ],
        compiler_params=pltpu.CompilerParams(vmem_limit_bytes=VMEM_BYTES),
        cost_estimate=pl.CostEstimate(flops=9 * 10**9, bytes_accessed=6 * 4 * order**2, transcendentals=0),
    )(in_vmem(mine), in_vmem(other), in_hbm(panel))


def factor_next(gram, strip=16):
    order = gram.shape[0]
    return pl.pallas_call(
        functools.partial(next_kernel, strip),
        out_shape=jax.ShapeDtypeStruct((order, order), jnp.float32),
        in_specs=[VMEM],
        out_specs=VMEM,
        scratch_shapes=[pltpu.VMEM((order, order), jnp.float32)],
        compiler_params=pltpu.CompilerParams(vmem_limit_bytes=VMEM_BYTES),
        cost_estimate=pl.CostEstimate(flops=8 * 10**9, bytes_accessed=2 * 4 * order**2, transcendentals=0),
    )(gram)


def split_kernel(stage, mine_a, mine_b, arrived_a, arrived_b, *chunk_refs):
    index = plane_index(stage)
    rows = chunk_refs[0].shape[0]
    cut = mine_a.shape[1]
    for step, chunk_ref in enumerate(chunk_refs):
        area = pl.ds(lax.rem(index + step, 4) * rows, rows)
        chunk_ref[:, :cut] = mine_a[area, :] + arrived_a[area, :]
        chunk_ref[:, cut:] = mine_b[area, :] + arrived_b[area, :]


def add_split(mine, arrived, stage):
    rows = mine[0].shape[0]
    width = mine[0].shape[1] + mine[1].shape[1]
    return pl.pallas_call(
        functools.partial(split_kernel, stage),
        out_shape=(jax.ShapeDtypeStruct((rows // 4, width), jnp.float32),) * 4,
        in_specs=[VMEM] * 4,
        out_specs=(VMEM,) * 4,
        compiler_params=pltpu.CompilerParams(vmem_limit_bytes=VMEM_BYTES),
        cost_estimate=pl.CostEstimate(flops=10**8, bytes_accessed=12 * rows * width, transcendentals=0),
    )(*(in_vmem(value) for value in (*mine, *arrived)))


def update_kernel(
    inv_rows, parts_ref, head_mine, head_other, rest_mine, rest_other, trailing_ref,
    proj_hbm, updated_hbm, proj_ref, updated_ref, sent,
):
    first = lax.axis_index("core") == 0
    width = parts_ref.shape[1]
    count = trailing_ref.shape[1] // width
    areas = [slice(width * t, width * t + width) for t in range(count)]
    inverse = [parts_ref[i] for i in range(3)]
    stores = []

    def project(tile):
        if tile == 0:
            halves = ordered(first, head_mine[:, areas[1]], head_other[:, areas[1]])
        else:
            halves = ordered(first, rest_mine[:, areas[tile - 1]], rest_other[:, areas[tile - 1]])
        proj = matmul(inverse, thirds(jnp.concatenate(halves, axis=0) * inv_rows))
        proj_ref[:, areas[tile]] = proj
        return thirds(proj)

    def send(source, target, tile, slot):
        copy = pltpu.make_async_copy(source.at[:, areas[tile]], target.at[:, areas[tile]], sent.at[slot])
        copy.start()
        stores.append(copy)

    ahead = project(0)
    basis = [parts_ref[i + 3] for i in range(3)]
    for tile in range(count):
        proj = ahead
        if tile + 1 < count:
            ahead = project(tile + 1)
        updated_ref[:, areas[tile]] = trailing_ref[:, areas[tile]] - matmul(basis, proj)
        send(proj_ref, proj_hbm, tile, 2 * tile)
        send(updated_ref, updated_hbm, tile, 2 * tile + 1)
    for copy in stores:
        copy.wait()


def update(parts, grams, rest, trailing, inv_rows):
    width = parts.shape[1]
    rows, columns = trailing.shape
    shapes = ((width, columns), (rows, columns))
    return pl.pallas_call(
        functools.partial(update_kernel, inv_rows),
        out_shape=tuple(jax.ShapeDtypeStruct(shape, jnp.float32) for shape in shapes),
        in_specs=[VMEM] * 6,
        out_specs=(HBM, HBM),
        scratch_shapes=[
            *(pltpu.VMEM(shape, jnp.float32) for shape in shapes),
            pltpu.SemaphoreType.DMA((2 * columns // width,)),
        ],
        compiler_params=pltpu.CompilerParams(vmem_limit_bytes=VMEM_BYTES),
        cost_estimate=pl.CostEstimate(flops=24 * rows * width * columns, bytes_accessed=16 * rows * columns, transcendentals=0),
    )(parts, *grams, *rest, trailing)


ROWS = ("y", "z", "core", "x")


def swap_cores(value):
    return lax.ppermute(value, "core", ((0, 1), (1, 0)))


def plane_shift(value, stage, step):
    pairs = []
    for y, z, core, x in itertools.product(range(4), range(8), range(2), range(4)):
        if core == stage:
            ny, nx = y, (x + step) % 4
        else:
            ny, nx = (y + step) % 4, x
        pairs.append((((y * 8 + z) * 2 + core) * 4 + x, ((ny * 8 + z) * 2 + core) * 4 + nx))
    return lax.ppermute(value, ROWS, pairs)


def plane_index(stage):
    return jnp.where(lax.axis_index("core") == stage, lax.axis_index("x"), lax.axis_index("y"))


def plane_sum(chunks, stage):
    total = chunks[0]
    for step in PLANE_STEPS:
        total = total + plane_shift(chunks[step], stage, step)
    return total


def plane_chunks(value, stage):
    chunks = value.reshape(4, value.shape[0] // 4, value.shape[1])
    index = plane_index(stage)
    return [
        lax.dynamic_index_in_dim(chunks, (index + step) % 4, 0, keepdims=False) for step in range(4)
    ]


def plane_send(value, stage):
    return [value] + [plane_shift(value, stage, step) for step in PLANE_STEPS]


def plane_join(pieces, stage):
    rows, width = pieces[0].shape
    index = plane_index(stage)
    result = jnp.zeros((4 * rows, width), pieces[0].dtype)
    for step, piece in zip((0, *PLANE_STEPS), pieces):
        result = lax.dynamic_update_slice(result, piece, ((index + 4 - step) % 4 * rows, 0))
    return result


def ring_sum(value):
    for bit in (4, 2, 1):
        value = value + lax.ppermute(value, "z", [(z, z ^ bit) for z in range(8)])
    return value


def per_device(panel, trailing):
    inv_rows = 1.0 / (panel.shape[0] * lax.axis_size(ROWS))
    width = panel.shape[1]
    mine_a, other_a, left, late = early_products(panel, trailing, 3 * width)
    arrived_a = swap_cores(other_a)
    mine_b, other_b = late_products(left, late)
    arrived_b = swap_cores(other_b)
    piece = plane_sum(add_split((mine_a, mine_b), (arrived_a, arrived_b), 0), 0)
    piece = ring_sum(plane_sum(plane_chunks(piece, 1), 1))
    piece = plane_join(plane_send(piece, 1), 1)
    gram_pieces = plane_send(piece[:, :3 * width], 0)
    rest_pieces = plane_send(piece[:, 3 * width:], 0)
    grams = plane_join(gram_pieces, 0)
    grams_other = swap_cores(grams)
    upper_panel, gram_next, parts = factor_panel(grams, grams_other, panel, inv_rows)
    rest_pieces, gram_next = lax.optimization_barrier((rest_pieces, gram_next))
    rest = plane_join(rest_pieces, 0)
    rest, gram_next = lax.optimization_barrier((rest, gram_next))
    rest_other = swap_cores(rest)
    upper_next = factor_next(gram_next)
    projection, updated = update(parts, (grams, grams_other), (rest, rest_other), trailing, inv_rows)
    return (upper_panel, projection, updated, upper_next)


def solution(mesh):
    chips = Mesh(mesh.devices.reshape(4, 8, 2, 4), ROWS)

    return jax.shard_map(
        per_device,
        mesh=chips,
        in_specs=(P(ROWS, None), P(ROWS, None)),
        out_specs=(P(), P(), P(ROWS, None), P()),
        check_vma=False,
    )
```
